128 devices in a mesh: chan: 16 (over x_lo, z, core), band: 8 (over y, x_hi).
Axes of the slice: x: 4 (x_hi: 2, x_lo: 2; x = x_hi * 2 + x_lo), y: 4, z: 4, core: 2. Of those that a mesh axis runs over, the one named last changes fastest.
Arguments:
- residual: float32 [128, 192, 16384], P('chan', 'band'), may hold values from -60 to 60
- weight_index: int32 [128], P('chan'), may hold values from 0 to 15
- weight_table: float32 [16], replicated, may hold values from 0.2 to 5
- gridded: float32 [2, 16, 256, 16384], P(None, 'chan', 'band'), may hold values from -6 to 6
Outputs:
- components: float32 [3, 192, 16384], P(None, 'band', 'chan')
- spectrum: float32 [2, 16, 16384, 256], P(None, 'chan', 'band')
The draws below stay inside these ranges and needn't reach their ends.
All inputs are finite; a program needn't handle non-finite values.
Results may differ from the reference program's by a relative error of at most 0.0002.
Values sent between devices are 32-bit elements; how exact they have to be, the bound alone decides.
A program may use at most 128 MiB of HBM per device.

```python
import math
import jax
import jax.numpy as jnp
from jax import lax

IMG = 16384
GRID = 16384
NW = 16
CHANNELS = 128
IMG_ROWS = 192
ROWS = 256
GROUPS = 16


def draw_residual(key, part):
    key_sky, key_noise = jax.random.split(jax.random.fold_in(key, 11), 2)
    position = jnp.arange(CHANNELS, dtype=jnp.float32)
    offset = (2.0 * position + 1.0) / CHANNELS - 1.0
    amplitude = jnp.array([1.0, 0.7, 0.5], dtype=jnp.float32)
    sky = jax.random.normal(key_sky, (3, IMG_ROWS, IMG), jnp.float32) * amplitude[:, None, None]
    noise = 3.0 * jax.random.normal(key_noise, (CHANNELS, IMG_ROWS, IMG), jnp.float32)
    values = sky[0][None] + offset[:, None, None] * sky[1][None] + (offset * offset)[:, None, None] * sky[2][None] + noise
    return jnp.clip(values, -60.0, 60.0)


def touch_ends(entries, rng, smallest, high):
    longest = entries.shape.index(max(entries.shape))
    spots = []
    for shift in (0, 1):
        where = [jax.random.randint(jax.random.fold_in(rng, axis), (), 0, length) for axis, length in enumerate(entries.shape)]
        where[longest] = (where[longest] + shift) % entries.shape[longest]
        spots.append(tuple(where))
    return entries.at[spots[0]].set(smallest).at[spots[1]].set(high)


def levels(stream_key, shape, cuts, low, top_value):
    def one(dim, blocks):
        heights = jax.random.uniform(jax.random.fold_in(jax.random.fold_in(stream_key, 6), dim), (blocks,), jnp.float32, low / len(cuts), top_value / len(cuts))
        return jnp.repeat(jnp.exp(heights), shape[dim] // blocks).reshape((-1,) + (1,) * (len(shape) - dim - 1))

    gain = one(*cuts[0])
    for cut in cuts[1:]:
        gain = gain * one(*cut)
    return gain


def normal_values(stream_key, shape, width, most, cuts=(), kind=jnp.bfloat16):
    values = width * jax.random.normal(stream_key, shape, jnp.float32)
    if cuts:
        values = values * levels(stream_key, shape, cuts, -0.22, 0.18)
    return jnp.clip(values, -most, most).astype(kind)


def setup_inputs(seed: int = 0) -> dict:
    key_of = jax.random.split(jax.random.key(seed), 5)
    return {
        "residual": draw_residual(jax.random.fold_in(key_of[4], 71), 0),
        "weight_index": touch_ends(jax.random.randint(key_of[1], (CHANNELS,), 0, NW), jax.random.fold_in(key_of[1], 1), 0, NW - 1).astype(jnp.int32),
        "weight_table": jnp.clip(jnp.exp(jax.random.uniform(key_of[2], (NW,), jnp.float32, math.log(0.2), math.log(5.0))), 0.2, 5.0),
        "gridded": normal_values(key_of[3], (2, GROUPS, ROWS, GRID), 1.0, 6.0, ((1, 16), (2, 8)), jnp.float32),
    }


def channel_terms(weight_index, weight_table, first, total):
    count = weight_index.shape[0]
    position = (first + jnp.arange(count, dtype=jnp.int32)).astype(jnp.float32)
    offset = (2.0 * position + 1.0) / total - 1.0
    slots = jnp.arange(weight_table.shape[0], dtype=jnp.int32)
    onehot = (weight_index[:, None] == slots[None, :]).astype(jnp.float32)
    weights = jnp.dot(onehot, weight_table, precision=lax.Precision.HIGHEST)
    return (weights, offset)

def solve_terms(moment, taylor):
    sum_zero, sum_one, sum_two, sum_three, sum_four = (moment[0], moment[1], moment[2], moment[3], moment[4])
    entry_aa = sum_two * sum_four - sum_three * sum_three
    entry_ab = sum_two * sum_three - sum_one * sum_four
    entry_ac = sum_one * sum_three - sum_two * sum_two
    entry_bb = sum_zero * sum_four - sum_two * sum_two
    entry_bc = sum_one * sum_two - sum_zero * sum_three
    entry_cc = sum_zero * sum_two - sum_one * sum_one
    determ = sum_zero * entry_aa + sum_one * entry_ab + sum_two * entry_ac
    inverse = jnp.stack([jnp.stack([entry_aa, entry_ab, entry_ac]), jnp.stack([entry_ab, entry_bb, entry_bc]), jnp.stack([entry_ac, entry_bc, entry_cc])]) / determ
    return jnp.einsum('ts,sij->tij', inverse, taylor, precision=lax.Precision.HIGHEST)

def reference(residual, weight_index, weight_table, gridded):
    weights, offset = channel_terms(weight_index, weight_table, 0, CHANNELS)
    coeffs = jnp.stack([weights, weights * offset, weights * offset * offset])
    flat = residual.reshape(residual.shape[0], -1)
    taylor = jnp.dot(coeffs, flat, precision=lax.Precision.HIGHEST).reshape(3, residual.shape[1], residual.shape[2])
    moment = jnp.stack([jnp.sum(weights * offset ** power) for power in range(5)])
    components = solve_terms(moment, taylor)
    field = gridded[0] + 1j * gridded[1]
    transformed = jnp.fft.fft(field, axis=-1) / jnp.sqrt(jnp.float32(GRID))
    stacked = jnp.stack([jnp.real(transformed), jnp.imag(transformed)]).astype(jnp.float32)
    spectrum = jnp.swapaxes(stacked, 2, 3)
    return (components, spectrum)
```

```python
import functools

import jax
import jax.numpy as jnp
import numpy as np
from jax import lax
from jax.experimental import pallas as pl
from jax.experimental.pallas import tpu as pltpu
from jax.sharding import PartitionSpec as P

MESH = pl.DeviceIdType.MESH
RADIX = 128
TERMS = 3
SHIFTS = (2, 1, 3, 0)


def tables():
    step = np.arange(RADIX)
    angle = 2.0 * np.pi * (np.outer(step, step) % RADIX) / RADIX
    cos, sin = (np.cos(angle), np.sin(angle))
    whole = np.block([[cos, sin], [-sin, cos]]).astype(np.float32)
    high = whole.astype(jnp.bfloat16)
    low = (whole - high.astype(np.float32)).astype(jnp.bfloat16)
    turn = 2.0 * np.pi * np.outer(step, step) / (RADIX * RADIX)
    twist_re = np.tile(np.cos(turn) / RADIX, (1, 2)).astype(np.float32)
    twist_im = np.tile(-np.sin(turn) / RADIX, (1, 2)).astype(np.float32)
    return (high, low, twist_re, twist_im)


def split_pair(value):
    high = value.astype(jnp.bfloat16)
    low = (value - high.astype(jnp.float32)).astype(jnp.bfloat16)
    return (high, low)


def three_products(high, low, value, dims):
    value_high, value_low = split_pair(value)
    mul = functools.partial(
        lax.dot_general, dimension_numbers=(dims, ((), ())), preferred_element_type=jnp.float32
    )
    return mul(high, value_high) + mul(high, value_low) + mul(low, value_high)


def solve_rows(moment, taylor):
    m0, m1, m2, m3, m4 = moment
    aa = m2 * m4 - m3 * m3
    ab = m2 * m3 - m1 * m4
    ac = m1 * m3 - m2 * m2
    bb = m0 * m4 - m2 * m2
    bc = m1 * m2 - m0 * m3
    cc = m0 * m2 - m1 * m1
    determ = m0 * aa + m1 * ab + m2 * ac
    aa, ab, ac, bb, bc, cc = (entry / determ for entry in (aa, ab, ac, bb, bc, cc))
    return ((aa, ab, ac), (ab, bb, bc), (ac, bc, cc))


def body(
    res_hbm, index_ref, table_ref, grid_hbm, high_ref, low_ref, tre_ref, tim_ref,
    comp_ref, spec_ref,
    grid_buf, res_buf, send_buf, recv_buf, core_send, own_buf, core_recv, z_recv, x_send, x_recv,
    grid_sem, res_sem, a_send, a_recv, c_send, c_recv, z_send_sem, z_recv_sem, x_send_sem, x_recv_sem,
):
    groups = lax.axis_size("chan")
    bands = lax.axis_size("band")
    zs = groups // 4
    chan = lax.axis_index("chan")
    band = lax.axis_index("band")
    x_lo = chan // (2 * zs)
    z_at = (chan // 2) % zs
    core = chan % 2
    count = res_hbm.shape[0]
    rows = res_hbm.shape[1]
    columns = res_hbm.shape[2] // groups
    row_tiles = rows // 8
    lane_tiles = columns // 128
    plane = row_tiles * lane_tiles
    blocks = grid_hbm.shape[1]
    pieces = send_buf.shape[1]
    halves = pieces // 2

    def chan_of(x, z, c):
        return (x * zs + z) * 2 + c

    def z_of(shift):
        return lax.rem(z_at + shift, zs)

    partner = {"chan": chan_of(x_lo, z_at, 1 - core)}
    across = {"chan": chan_of(1 - x_lo, z_at, core)}

    barrier = pltpu.get_barrier_semaphore()
    for shift in range(1, bands):
        pl.semaphore_signal(barrier, 1, device_id={"band": lax.rem(band + shift, bands)}, device_id_type=MESH)
    for shift in SHIFTS[:-1]:
        pl.semaphore_signal(barrier, 1, device_id={"chan": chan_of(x_lo, z_of(shift), core)}, device_id_type=MESH)
    pl.semaphore_signal(barrier, 1, device_id=partner, device_id_type=MESH)
    pl.semaphore_signal(barrier, 1, device_id=across, device_id_type=MESH)

    grid_copies = [
        pltpu.make_async_copy(grid_hbm.at[:, k], grid_buf.at[:, k], grid_sem.at[k]) for k in range(blocks)
    ]
    for copy in grid_copies:
        copy.start()
    slots = [(other, shift) for other in (1, 0) for shift in SHIFTS]
    order = [(away, slot) for away in (1, 0) for slot in range(len(slots))]

    def block_of(away, slot):
        other, shift = slots[slot]
        return chan_of((x_lo + other) % 2, z_of(shift), (core + away) % 2)

    res_copies = []
    for k, (away, slot) in enumerate(order):
        start = pl.multiple_of(block_of(away, slot) * columns, columns)
        res_copies.append(
            pltpu.make_async_copy(res_hbm.at[:, :, pl.ds(start, columns)], res_buf.at[k], res_sem.at[k])
        )
    for copy in res_copies:
        copy.start()

    for block in range(blocks):
        grid_copies[block].wait()

        def pair(step, carry, block=block):
            def taken(part, row):
                return grid_buf[part, block, pl.ds(row, RADIX, stride=8), :]

            first = step * 2
            value = jnp.concatenate(
                [
                    jnp.concatenate([taken(0, first), taken(0, first + 1)], axis=1),
                    jnp.concatenate([taken(1, first), taken(1, first + 1)], axis=1),
                ],
                axis=0,
            )
            high, low = (high_ref[...], low_ref[...])
            stage = three_products(high, low, value, ((1,), (0,)))
            real, imag = (stage[:RADIX], stage[RADIX:])
            tre, tim = (tre_ref[...], tim_ref[...])
            turned_re = real * tre - imag * tim
            turned_im = real * tim + imag * tre
            turned = jnp.concatenate(
                [
                    jnp.concatenate([turned_re[:, :RADIX], turned_im[:, :RADIX]], axis=1),
                    jnp.concatenate([turned_re[:, RADIX:], turned_im[:, RADIX:]], axis=1),
                ],
                axis=0,
            )
            final = three_products(high, low, turned, ((1,), (1,)))
            for half_row in range(2):
                row = block * 8 + first + half_row
                for target in range(bands):
                    for part in range(2):
                        for half in range(halves):
                            at = part * RADIX + target * (8 * halves) + half * 8
                            start = pl.multiple_of(row * 8, 8)
                            send_buf[target, half * 2 + part, pl.ds(start, 8), :] = final[
                                at : at + 8, half_row * RADIX : (half_row + 1) * RADIX
                            ]
            return carry

        lax.fori_loop(0, 4, pair, 0)

    peers = 7 + len(SHIFTS) - 1 + 2
    pl.semaphore_wait(barrier, peers)

    def spectrum_copy(piece, shift):
        target = lax.rem(band + shift, bands)
        at = piece * bands + shift
        return pltpu.make_async_remote_copy(
            src_ref=send_buf.at[target, piece],
            dst_ref=recv_buf.at[piece, band],
            send_sem=a_send.at[at],
            recv_sem=a_recv.at[at],
            device_id={"band": target},
            device_id_type=MESH,
        )

    spectrum_copies = [[spectrum_copy(piece, shift) for shift in range(1, bands)] for piece in range(pieces)]
    for piece in range(pieces):
        for copy in spectrum_copies[piece]:
            copy.start()

    weights, offsets = ([], [])
    for k in range(count):
        weights.append(table_ref[index_ref[k]])
        position = (chan * count + k).astype(jnp.float32)
        offsets.append((2.0 * position + 1.0) / (count * groups) - 1.0)
    coeffs = [weights, [w * o for w, o in zip(weights, offsets)], [w * o * o for w, o in zip(weights, offsets)]]
    powers = list(weights)
    moments = []
    for power in range(5):
        total = powers[0]
        for k in range(1, count):
            total = total + powers[k]
        moments.append(total)
        powers = [p * o for p, o in zip(powers, offsets)]
    sublane = lax.broadcasted_iota(jnp.int32, (8, 128), 0)
    moment_tile = jnp.zeros((8, 128), jnp.float32)
    for power in range(5):
        moment_tile = jnp.where(sublane == power, moments[power], moment_tile)

    def sums(k, target_ref, slot, extra):
        res_copies[k].wait()

        def tile(step, carry):
            row = step // lane_tiles
            lane = lax.rem(step, lane_tiles)
            rows_at = pl.ds(pl.multiple_of(row * 8, 8), 8)
            lanes_at = pl.ds(pl.multiple_of(lane * 128, 128), 128)
            totals = [None] * TERMS
            for channel in range(count):
                value = res_buf[k, channel, rows_at, lanes_at]
                for term in range(TERMS):
                    product = value * coeffs[term][channel]
                    totals[term] = product if totals[term] is None else totals[term] + product
            for term in range(TERMS):
                at = term * plane + step
                total = totals[term]
                if extra is not None:
                    total = total + extra[slot, at]
                target_ref[slot, at] = total
            return carry

        lax.fori_loop(0, plane, tile, 0, unroll=4)
        moment = moment_tile
        if extra is not None:
            moment = moment + extra[slot, TERMS * plane]
        target_ref[slot, TERMS * plane] = moment

    core_copies = []
    for slot in range(len(slots)):
        sums(slot, core_send, slot, None)
        copy = pltpu.make_async_remote_copy(
            src_ref=core_send.at[slot],
            dst_ref=core_recv.at[slot],
            send_sem=c_send.at[slot],
            recv_sem=c_recv.at[slot],
            device_id=partner,
            device_id_type=MESH,
        )
        copy.start()
        core_copies.append(copy)

    z_copies = {}
    for slot, (other, shift) in enumerate(slots):
        core_copies[slot].wait_recv()
        sums(len(slots) + slot, own_buf, slot, core_recv)
        if shift:
            copy = pltpu.make_async_remote_copy(
                src_ref=own_buf.at[slot],
                dst_ref=z_recv.at[slot],
                send_sem=z_send_sem.at[slot],
                recv_sem=z_recv_sem.at[slot],
                device_id={"chan": chan_of(x_lo, z_of(shift), core)},
                device_id_type=MESH,
            )
            copy.start()
            z_copies[slot] = copy

    own = send_buf.at[band]
    for piece in range(pieces):
        recv_buf[piece, band] = own[piece]

    def gathered(other, target):
        base = [k for k, key in enumerate(slots) if key == (other, 0)][0]
        came = [k for k, key in enumerate(slots) if key[0] == other and key[1]]
        for slot in came:
            z_copies[slot].wait_recv()

        def tile(step, carry):
            total = own_buf[base, step]
            for slot in came:
                total = total + z_recv[slot, step]
            target[step] = total
            return carry

        lax.fori_loop(0, TERMS * plane + 1, tile, 0)

    gathered(1, x_send)
    x_copy = pltpu.make_async_remote_copy(
        src_ref=x_send,
        dst_ref=x_recv,
        send_sem=x_send_sem,
        recv_sem=x_recv_sem,
        device_id=across,
        device_id_type=MESH,
    )
    x_copy.start()

    def place(piece):
        half, part = divmod(piece, 2)
        for copy in spectrum_copies[piece]:
            copy.wait_recv()

        def turn(k, carry):
            for side in range(2):
                value = jnp.concatenate(
                    [recv_buf[piece, side * 4 + source, pl.ds(k, 32, stride=8), :] for source in range(4)],
                    axis=0,
                )
                start = pl.multiple_of((half * 8 + k) * RADIX, RADIX)
                spec_ref[part, pl.ds(start, RADIX), pl.ds(side * 128, 128)] = value.T
            return carry

        lax.fori_loop(0, 8, turn, 0)

    def finish():
        gathered(0, own_buf.at[len(slots) - 1])
        x_copy.wait_recv()
        last = len(slots) - 1
        total = own_buf[last, TERMS * plane] + x_recv[TERMS * plane]
        inverse = solve_rows([total[k : k + 1] for k in range(5)], None)

        def tile(step, carry):
            row = step // lane_tiles
            lane = lax.rem(step, lane_tiles)
            rows_at = pl.ds(pl.multiple_of(row * 8, 8), 8)
            lanes_at = pl.ds(pl.multiple_of(lane * 128, 128), 128)
            taylor = [own_buf[last, s * plane + step] + x_recv[s * plane + step] for s in range(TERMS)]
            for t in range(TERMS):
                comp_ref[t, rows_at, lanes_at] = (
                    inverse[t][0] * taylor[0] + inverse[t][1] * taylor[1] + inverse[t][2] * taylor[2]
                )
            return carry

        lax.fori_loop(0, plane, tile, 0)

    for piece in range(pieces - 1):
        place(piece)
    finish()
    place(pieces - 1)

    for piece in range(pieces):
        for copy in spectrum_copies[piece]:
            copy.wait_send()
    for copy in core_copies:
        copy.wait_send()
    for copy in z_copies.values():
        copy.wait_send()
    x_copy.wait_send()


def local(residual, weight_index, weight_table, gridded):
    bands = lax.axis_size("band")
    groups = lax.axis_size("chan")
    count, rows, width = residual.shape
    grid_rows, length = gridded.shape[2:]
    blocks = grid_rows // 8
    tiled = gridded.reshape(2, blocks, 8, RADIX, RADIX)
    tiled = jnp.transpose(tiled, (0, 1, 3, 2, 4)).reshape(2, blocks, RADIX * 8, RADIX)
    columns = width // groups
    out_length = length // bands
    pieces = 2 * (RADIX // bands // 8)
    tiles = TERMS * (rows // 8) * (columns // 128) + 1
    f32 = jnp.float32
    any_space = pl.BlockSpec(memory_space=pl.ANY)
    vmem = pl.BlockSpec(memory_space=pltpu.VMEM)
    smem = pl.BlockSpec(memory_space=pltpu.SMEM)
    dma = pltpu.SemaphoreType.DMA
    slots = 2 * len(SHIFTS)
    components, spectrum = pl.pallas_call(
        body,
        out_shape=(
            pltpu.VMEM((TERMS, rows, columns), f32),
            pltpu.VMEM((2, out_length, grid_rows * bands), f32),
        ),
        in_specs=[any_space, smem, smem, any_space, vmem, vmem, vmem, vmem],
        out_specs=(vmem, vmem),
        scratch_shapes=[
            pltpu.VMEM((2, blocks, RADIX * 8, RADIX), f32),
            pltpu.VMEM((groups, count, rows, columns), f32),
            pltpu.VMEM((bands, pieces, grid_rows * 8, RADIX), f32),
            pltpu.VMEM((pieces, bands, grid_rows * 8, RADIX), f32),
            pltpu.VMEM((slots, tiles, 8, 128), f32),
            pltpu.VMEM((slots, tiles, 8, 128), f32),
            pltpu.VMEM((slots, tiles, 8, 128), f32),
            pltpu.VMEM((slots, tiles, 8, 128), f32),
            pltpu.VMEM((tiles, 8, 128), f32),
            pltpu.VMEM((tiles, 8, 128), f32),
            dma((blocks,)),
            dma((groups,)),
            dma((pieces * bands,)),
            dma((pieces * bands,)),
            dma((slots,)),
            dma((slots,)),
            dma((slots,)),
            dma((slots,)),
            dma,
            dma,
        ],
        compiler_params=pltpu.CompilerParams(
            collective_id=0, has_side_effects=True, vmem_limit_bytes=52 << 20
        ),
    )(residual, weight_index, weight_table, tiled, *(jnp.asarray(table) for table in tables()))
    return (components, spectrum.reshape(2, 1, out_length, grid_rows * bands))


def solution(mesh):
    in_specs = (P("chan", "band", None), P("chan"), P(), P(None, "chan", "band", None))
    out_specs = (P(None, "band", "chan"), P(None, "chan", "band", None))
    return jax.shard_map(local, mesh=mesh, in_specs=in_specs, out_specs=out_specs, check_vma=False)
```

```python
import functools

import jax
import jax.numpy as jnp
import numpy as np
from jax import lax
from jax.experimental import pallas as pl
from jax.experimental.pallas import tpu as pltpu
from jax.sharding import PartitionSpec as P

MESH = pl.DeviceIdType.MESH
RADIX = 128
TERMS = 3
SHIFTS = (2, 1, 3, 0)


def tables():
    step = np.arange(RADIX)
    angle = 2.0 * np.pi * (np.outer(step, step) % RADIX) / RADIX
    cos, sin = (np.cos(angle), np.sin(angle))
    whole = np.block([[cos, sin], [-sin, cos]]).astype(np.float32)
    high = whole.astype(jnp.bfloat16)
    low = (whole - high.astype(np.float32)).astype(jnp.bfloat16)
    turn = 2.0 * np.pi * np.outer(step, step) / (RADIX * RADIX)
    twist = np.stack([np.cos(turn), -np.sin(turn)]) / RADIX
    return (np.concatenate([high, low]), twist.astype(np.float32))


def three_products(pair, value, axis):
    width = 2 * RADIX
    mul = functools.partial(
        lax.dot_general,
        dimension_numbers=(((1,), (axis,)), ((), ())),
        preferred_element_type=jnp.float32,
    )
    done = []
    for k in range(value.shape[1 - axis] // width):
        cut = slice(k * width, (k + 1) * width)
        tile = value[:, cut] if axis == 0 else value[cut]
        high = tile.astype(jnp.bfloat16)
        low = (tile - high.astype(jnp.float32)).astype(jnp.bfloat16)
        both = mul(pair, high)
        done.append(both[:width] + (both[width:] + mul(pair[:width], low)))
    return jnp.concatenate(done, axis=1)


def solve_rows(moment, taylor):
    m0, m1, m2, m3, m4 = moment
    aa = m2 * m4 - m3 * m3
    ab = m2 * m3 - m1 * m4
    ac = m1 * m3 - m2 * m2
    bb = m0 * m4 - m2 * m2
    bc = m1 * m2 - m0 * m3
    cc = m0 * m2 - m1 * m1
    determ = m0 * aa + m1 * ab + m2 * ac
    aa, ab, ac, bb, bc, cc = (entry / determ for entry in (aa, ab, ac, bb, bc, cc))
    return ((aa, ab, ac), (ab, bb, bc), (ac, bc, cc))


def body(
    res_hbm, index_hbm, table_hbm, grid_hbm, pair_hbm, twist_hbm,
    comp_ref, spec_ref,
    index_ref, table_ref, pair_ref, twist_ref, grid_buf, res_buf, send_buf, recv_buf, core_send, own_buf, core_recv, z_recv, x_send, x_recv,
    small_sem, grid_sem, res_sem, a_send, a_recv, c_send, c_recv, z_send_sem, z_recv_sem, x_send_sem, x_recv_sem,
):
    groups = lax.axis_size("chan")
    bands = lax.axis_size("band")
    zs = groups // 4
    chan = lax.axis_index("chan")
    band = lax.axis_index("band")
    x_lo = chan // (2 * zs)
    z_at = (chan // 2) % zs
    core = chan % 2
    count = res_hbm.shape[0]
    rows = res_hbm.shape[1]
    columns = res_hbm.shape[2] // groups
    row_tiles = rows // 8
    lane_tiles = columns // 128
    plane = row_tiles * lane_tiles
    blocks = grid_hbm.shape[1]
    pieces = send_buf.shape[1]
    halves = pieces // 2

    def chan_of(x, z, c):
        return (x * zs + z) * 2 + c

    def z_of(shift):
        return lax.rem(z_at + shift, zs)

    partner = {"chan": chan_of(x_lo, z_at, 1 - core)}
    across = {"chan": chan_of(1 - x_lo, z_at, core)}

    barrier = pltpu.get_barrier_semaphore()
    for shift in range(1, bands):
        pl.semaphore_signal(barrier, 1, device_id={"band": lax.rem(band + shift, bands)}, device_id_type=MESH)
    for shift in SHIFTS[:-1]:
        pl.semaphore_signal(barrier, 1, device_id={"chan": chan_of(x_lo, z_of(shift), core)}, device_id_type=MESH)
    pl.semaphore_signal(barrier, 1, device_id=partner, device_id_type=MESH)
    pl.semaphore_signal(barrier, 1, device_id=across, device_id_type=MESH)

    grid_copies = [
        pltpu.make_async_copy(grid_hbm.at[:, k], grid_buf.at[:, k], grid_sem.at[k]) for k in range(blocks)
    ]
    small_copies = [
        pltpu.make_async_copy(source, target, small_sem.at[k])
        for k, (source, target) in enumerate(
            ((pair_hbm, pair_ref), (twist_hbm, twist_ref), (index_hbm, index_ref), (table_hbm, table_ref))
        )
    ]
    for copy in (grid_copies[0], *small_copies, *grid_copies[1:]):
        copy.start()
    slots = [(other, shift) for other in (1, 0) for shift in SHIFTS]
    order = [(away, slot) for away in (1, 0) for slot in range(len(slots))]

    def block_of(away, slot):
        other, shift = slots[slot]
        return chan_of((x_lo + other) % 2, z_of(shift), (core + away) % 2)

    res_copies = []
    for k, (away, slot) in enumerate(order):
        start = pl.multiple_of(block_of(away, slot) * columns, columns)
        res_copies.append(
            pltpu.make_async_copy(res_hbm.at[:, :, pl.ds(start, columns)], res_buf.at[k], res_sem.at[k])
        )
    for copy in res_copies:
        copy.start()

    for copy in small_copies:
        copy.wait()

    def transform(block, carry):
        def taken(part):
            return jnp.concatenate([grid_buf[part, block, pl.ds(k, RADIX, stride=8), :] for k in range(8)], axis=1)

        pair = pair_ref[...]
        stage = three_products(pair, jnp.concatenate([taken(0), taken(1)], axis=0), 0)
        tre, tim = (twist_ref[0], twist_ref[1])
        turned = []
        for k in range(8):
            cut = slice(k * RADIX, (k + 1) * RADIX)
            real, imag = (stage[:RADIX, cut], stage[RADIX:, cut])
            turned.append(jnp.concatenate([real * tre - imag * tim, real * tim + imag * tre], axis=1))
        final = three_products(pair, jnp.concatenate(turned, axis=0), 1)
        for k in range(8):
            start = pl.multiple_of(block * 64 + k * 8, 8)
            for target in range(bands):
                for part in range(2):
                    for half in range(halves):
                        at = part * RADIX + target * (8 * halves) + half * 8
                        send_buf[target, half * 2 + part, pl.ds(start, 8), :] = final[
                            at : at + 8, k * RADIX : (k + 1) * RADIX
                        ]
        return carry

    for block in range(blocks):
        grid_copies[block].wait()
        transform(block, 0)

    peers = 7 + len(SHIFTS) - 1 + 2
    pl.semaphore_wait(barrier, peers)

    def spectrum_copy(piece, shift):
        target = lax.rem(band + shift, bands)
        at = piece * bands + shift
        return pltpu.make_async_remote_copy(
            src_ref=send_buf.at[target, piece],
            dst_ref=recv_buf.at[piece, band],
            send_sem=a_send.at[at],
            recv_sem=a_recv.at[at],
            device_id={"band": target},
            device_id_type=MESH,
        )

    spectrum_copies = [[spectrum_copy(piece, shift) for shift in range(1, bands)] for piece in range(pieces)]
    for piece in range(pieces):
        for copy in spectrum_copies[piece]:
            copy.start()

    weights, offsets = ([], [])
    for k in range(count):
        weights.append(table_ref[index_ref[k]])
        position = (chan * count + k).astype(jnp.float32)
        offsets.append((2.0 * position + 1.0) / (count * groups) - 1.0)
    coeffs = [weights, [w * o for w, o in zip(weights, offsets)], [w * o * o for w, o in zip(weights, offsets)]]
    powers = list(weights)
    moments = []
    for power in range(5):
        total = powers[0]
        for k in range(1, count):
            total = total + powers[k]
        moments.append(total)
        powers = [p * o for p, o in zip(powers, offsets)]
    sublane = lax.broadcasted_iota(jnp.int32, (8, 128), 0)
    moment_tile = jnp.zeros((8, 128), jnp.float32)
    for power in range(5):
        moment_tile = jnp.where(sublane == power, moments[power], moment_tile)

    def sums(k, target_ref, slot, extra):
        res_copies[k].wait()

        def tile(step, carry):
            row = step // lane_tiles
            lane = lax.rem(step, lane_tiles)
            rows_at = pl.ds(pl.multiple_of(row * 8, 8), 8)
            lanes_at = pl.ds(pl.multiple_of(lane * 128, 128), 128)
            totals = [None] * TERMS
            for channel in range(count):
                value = res_buf[k, channel, rows_at, lanes_at]
                for term in range(TERMS):
                    product = value * coeffs[term][channel]
                    totals[term] = product if totals[term] is None else totals[term] + product
            for term in range(TERMS):
                at = term * plane + step
                total = totals[term]
                if extra is not None:
                    total = total + extra[slot, at]
                target_ref[slot, at] = total
            return carry

        lax.fori_loop(0, plane, tile, 0, unroll=4)
        moment = moment_tile
        if extra is not None:
            moment = moment + extra[slot, TERMS * plane]
        target_ref[slot, TERMS * plane] = moment

    core_copies = []
    for slot in range(len(slots)):
        sums(slot, core_send, slot, None)
        copy = pltpu.make_async_remote_copy(
            src_ref=core_send.at[slot],
            dst_ref=core_recv.at[slot],
            send_sem=c_send.at[slot],
            recv_sem=c_recv.at[slot],
            device_id=partner,
            device_id_type=MESH,
        )
        copy.start()
        core_copies.append(copy)

    z_copies = {}
    for slot, (other, shift) in enumerate(slots):
        core_copies[slot].wait_recv()
        sums(len(slots) + slot, own_buf, slot, core_recv)
        if shift:
            copy = pltpu.make_async_remote_copy(
                src_ref=own_buf.at[slot],
                dst_ref=z_recv.at[slot],
                send_sem=z_send_sem.at[slot],
                recv_sem=z_recv_sem.at[slot],
                device_id={"chan": chan_of(x_lo, z_of(shift), core)},
                device_id_type=MESH,
            )
            copy.start()
            z_copies[slot] = copy

    own = send_buf.at[band]
    for piece in range(pieces):
        recv_buf[piece, band] = own[piece]

    def gathered(other, target):
        base = [k for k, key in enumerate(slots) if key == (other, 0)][0]
        came = [k for k, key in enumerate(slots) if key[0] == other and key[1]]
        for slot in came:
            z_copies[slot].wait_recv()

        def tile(step, carry):
            total = own_buf[base, step]
            for slot in came:
                total = total + z_recv[slot, step]
            target[step] = total
            return carry

        lax.fori_loop(0, TERMS * plane + 1, tile, 0)

    gathered(1, x_send)
    x_copy = pltpu.make_async_remote_copy(
        src_ref=x_send,
        dst_ref=x_recv,
        send_sem=x_send_sem,
        recv_sem=x_recv_sem,
        device_id=across,
        device_id_type=MESH,
    )
    x_copy.start()

    def place(piece):
        half, part = divmod(piece, 2)
        for copy in spectrum_copies[piece]:
            copy.wait_recv()

        def turn(k, carry):
            for side in range(2):
                value = jnp.concatenate(
                    [recv_buf[piece, side * 4 + source, pl.ds(k, 32, stride=8), :] for source in range(4)],
                    axis=0,
                )
                start = pl.multiple_of((half * 8 + k) * RADIX, RADIX)
                spec_ref[part, pl.ds(start, RADIX), pl.ds(side * 128, 128)] = value.T
            return carry

        lax.fori_loop(0, 8, turn, 0)

    def finish():
        gathered(0, own_buf.at[len(slots) - 1])
        x_copy.wait_recv()
        last = len(slots) - 1
        total = own_buf[last, TERMS * plane] + x_recv[TERMS * plane]
        inverse = solve_rows([total[k : k + 1] for k in range(5)], None)

        def tile(step, carry):
            row = step // lane_tiles
            lane = lax.rem(step, lane_tiles)
            rows_at = pl.ds(pl.multiple_of(row * 8, 8), 8)
            lanes_at = pl.ds(pl.multiple_of(lane * 128, 128), 128)
            taylor = [own_buf[last, s * plane + step] + x_recv[s * plane + step] for s in range(TERMS)]
            for t in range(TERMS):
                comp_ref[t, rows_at, lanes_at] = (
                    inverse[t][0] * taylor[0] + inverse[t][1] * taylor[1] + inverse[t][2] * taylor[2]
                )
            return carry

        lax.fori_loop(0, plane, tile, 0)

    for piece in range(pieces - 1):
        place(piece)
    finish()
    place(pieces - 1)

    for piece in range(pieces):
        for copy in spectrum_copies[piece]:
            copy.wait_send()
    for copy in core_copies:
        copy.wait_send()
    for copy in z_copies.values():
        copy.wait_send()
    x_copy.wait_send()


def local(residual, weight_index, weight_table, gridded):
    bands = lax.axis_size("band")
    groups = lax.axis_size("chan")
    count, rows, width = residual.shape
    grid_rows, length = gridded.shape[2:]
    blocks = grid_rows // 8
    tiled = gridded.reshape(2, blocks, 8, RADIX, RADIX)
    tiled = jnp.transpose(tiled, (0, 1, 3, 2, 4)).reshape(2, blocks, RADIX * 8, RADIX)
    columns = width // groups
    out_length = length // bands
    pieces = 2 * (RADIX // bands // 8)
    tiles = TERMS * (rows // 8) * (columns // 128) + 1
    f32 = jnp.float32
    any_space = pl.BlockSpec(memory_space=pl.ANY)
    vmem = pl.BlockSpec(memory_space=pltpu.VMEM)
    dma = pltpu.SemaphoreType.DMA
    slots = 2 * len(SHIFTS)
    components, spectrum = pl.pallas_call(
        body,
        out_shape=(
            pltpu.VMEM((TERMS, rows, columns), f32),
            pltpu.VMEM((2, out_length, grid_rows * bands), f32),
        ),
        in_specs=[any_space] * 6,
        out_specs=(vmem, vmem),
        scratch_shapes=[
            pltpu.SMEM(weight_index.shape, weight_index.dtype),
            pltpu.SMEM(weight_table.shape, f32),
            pltpu.VMEM((4 * RADIX, 2 * RADIX), jnp.bfloat16),
            pltpu.VMEM((2, RADIX, RADIX), f32),
            pltpu.VMEM((2, blocks, RADIX * 8, RADIX), f32),
            pltpu.VMEM((groups, count, rows, columns), f32),
            pltpu.VMEM((bands, pieces, grid_rows * 8, RADIX), f32),
            pltpu.VMEM((pieces, bands, grid_rows * 8, RADIX), f32),
            pltpu.VMEM((slots, tiles, 8, 128), f32),
            pltpu.VMEM((slots, tiles, 8, 128), f32),
            pltpu.VMEM((slots, tiles, 8, 128), f32),
            pltpu.VMEM((slots, tiles, 8, 128), f32),
            pltpu.VMEM((tiles, 8, 128), f32),
            pltpu.VMEM((tiles, 8, 128), f32),
            dma((4,)),
            dma((blocks,)),
            dma((groups,)),
            dma((pieces * bands,)),
            dma((pieces * bands,)),
            dma((slots,)),
            dma((slots,)),
            dma((slots,)),
            dma((slots,)),
            dma,
            dma,
        ],
        compiler_params=pltpu.CompilerParams(
            collective_id=0, has_side_effects=True, vmem_limit_bytes=52 << 20
        ),
    )(residual, weight_index, weight_table, tiled, *(jnp.asarray(table) for table in tables()))
    return (components, spectrum.reshape(2, 1, out_length, grid_rows * bands))


def solution(mesh):
    in_specs = (P("chan", "band", None), P("chan"), P(), P(None, "chan", "band", None))
    out_specs = (P(None, "band", "chan"), P(None, "chan", "band", None))
    return jax.shard_map(local, mesh=mesh, in_specs=in_specs, out_specs=out_specs, check_vma=False)
```

```python
import functools

import jax
import jax.numpy as jnp
import numpy as np
from jax import lax
from jax.experimental import pallas as pl
from jax.experimental.pallas import tpu as pltpu
from jax.sharding import PartitionSpec as P

MESH = pl.DeviceIdType.MESH
RADIX = 128
TERMS = 3
SHIFTS = (2, 1, 3, 0)


def tables():
    step = np.arange(RADIX)
    angle = 2.0 * np.pi * (np.outer(step, step) % RADIX) / RADIX
    cos, sin = (np.cos(angle), np.sin(angle))
    whole = np.block([[cos, sin], [-sin, cos]]).astype(np.float32)
    high = whole.astype(jnp.bfloat16)
    low = (whole - high.astype(np.float32)).astype(jnp.bfloat16)
    turn = 2.0 * np.pi * np.outer(step, step) / (RADIX * RADIX)
    twist = np.stack([np.cos(turn), -np.sin(turn)]) / RADIX
    return (np.concatenate([high, low]), twist.astype(np.float32))


def three_products(pair, value, axis):
    width = 2 * RADIX
    mul = functools.partial(
        lax.dot_general,
        dimension_numbers=(((1,), (axis,)), ((), ())),
        preferred_element_type=jnp.float32,
    )
    done = []
    for k in range(value.shape[1 - axis] // width):
        cut = slice(k * width, (k + 1) * width)
        tile = value[:, cut] if axis == 0 else value[cut]
        high = tile.astype(jnp.bfloat16)
        low = (tile - high.astype(jnp.float32)).astype(jnp.bfloat16)
        both = mul(pair, high)
        done.append(both[:width] + (both[width:] + mul(pair[:width], low)))
    return jnp.concatenate(done, axis=1)


def solve_rows(moment, taylor):
    m0, m1, m2, m3, m4 = moment
    aa = m2 * m4 - m3 * m3
    ab = m2 * m3 - m1 * m4
    ac = m1 * m3 - m2 * m2
    bb = m0 * m4 - m2 * m2
    bc = m1 * m2 - m0 * m3
    cc = m0 * m2 - m1 * m1
    determ = m0 * aa + m1 * ab + m2 * ac
    aa, ab, ac, bb, bc, cc = (entry / determ for entry in (aa, ab, ac, bb, bc, cc))
    return ((aa, ab, ac), (ab, bb, bc), (ac, bc, cc))


def body(
    res_hbm, index_hbm, table_hbm, grid_hbm, pair_hbm, twist_hbm,
    comp_ref, spec_ref,
    index_ref, table_ref, pair_ref, twist_ref, grid_buf, res_buf, send_buf, recv_buf, core_send, own_buf, core_recv, z_recv, x_send, x_recv,
    small_sem, grid_sem, res_sem, a_send, a_recv, c_send, c_recv, z_send_sem, z_recv_sem, x_send_sem, x_recv_sem,
):
    groups = lax.axis_size("chan")
    bands = lax.axis_size("band")
    zs = groups // 4
    chan = lax.axis_index("chan")
    band = lax.axis_index("band")
    x_lo = chan // (2 * zs)
    z_at = (chan // 2) % zs
    core = chan % 2
    count = res_hbm.shape[0]
    rows = res_hbm.shape[1]
    columns = res_hbm.shape[2] // groups
    row_tiles = rows // 8
    lane_tiles = columns // 128
    plane = row_tiles * lane_tiles
    blocks = grid_hbm.shape[1]
    pieces = send_buf.shape[1]
    halves = pieces // 2

    def chan_of(x, z, c):
        return (x * zs + z) * 2 + c

    def z_of(shift):
        return lax.rem(z_at + shift, zs)

    partner = {"chan": chan_of(x_lo, z_at, 1 - core)}
    across = {"chan": chan_of(1 - x_lo, z_at, core)}

    barrier = pltpu.get_barrier_semaphore()
    for shift in range(1, bands):
        pl.semaphore_signal(barrier, 1, device_id={"band": lax.rem(band + shift, bands)}, device_id_type=MESH)
    for shift in SHIFTS[:-1]:
        pl.semaphore_signal(barrier, 1, device_id={"chan": chan_of(x_lo, z_of(shift), core)}, device_id_type=MESH)
    pl.semaphore_signal(barrier, 1, device_id=partner, device_id_type=MESH)
    pl.semaphore_signal(barrier, 1, device_id=across, device_id_type=MESH)

    grid_copies = [
        pltpu.make_async_copy(grid_hbm.at[:, k], grid_buf.at[:, k], grid_sem.at[k]) for k in range(blocks)
    ]
    small_copies = [
        pltpu.make_async_copy(source, target, small_sem.at[k])
        for k, (source, target) in enumerate(
            ((pair_hbm, pair_ref), (twist_hbm, twist_ref), (index_hbm, index_ref), (table_hbm, table_ref))
        )
    ]
    for copy in (grid_copies[0], *small_copies, *grid_copies[1:]):
        copy.start()
    slots = [(other, shift) for other in (1, 0) for shift in SHIFTS]
    order = [(away, slot) for away in (1, 0) for slot in range(len(slots))]

    def block_of(away, slot):
        other, shift = slots[slot]
        return chan_of((x_lo + other) % 2, z_of(shift), (core + away) % 2)

    res_copies = []
    for k, (away, slot) in enumerate(order):
        start = pl.multiple_of(block_of(away, slot) * columns, columns)
        res_copies.append(
            pltpu.make_async_copy(res_hbm.at[:, :, pl.ds(start, columns)], res_buf.at[k], res_sem.at[k])
        )

    for copy in small_copies:
        copy.wait()

    def transform(block, carry):
        def taken(part):
            return jnp.concatenate([grid_buf[part, block, pl.ds(k, RADIX, stride=8), :] for k in range(8)], axis=1)

        pair = pair_ref[...]
        stage = three_products(pair, jnp.concatenate([taken(0), taken(1)], axis=0), 0)
        tre, tim = (twist_ref[0], twist_ref[1])
        turned = []
        for k in range(8):
            cut = slice(k * RADIX, (k + 1) * RADIX)
            real, imag = (stage[:RADIX, cut], stage[RADIX:, cut])
            turned.append(jnp.concatenate([real * tre - imag * tim, real * tim + imag * tre], axis=1))
        final = three_products(pair, jnp.concatenate(turned, axis=0), 1)
        for k in range(8):
            start = pl.multiple_of(block * 64 + k * 8, 8)
            for target in range(bands):
                for part in range(2):
                    for half in range(halves):
                        at = part * RADIX + target * (8 * halves) + half * 8
                        send_buf[target, half * 2 + part, pl.ds(start, 8), :] = final[
                            at : at + 8, k * RADIX : (k + 1) * RADIX
                        ]
        return carry

    for block in range(blocks):
        grid_copies[block].wait()
        if block == blocks - 1:
            for copy in res_copies:
                copy.start()
        transform(block, 0)

    peers = 7 + len(SHIFTS) - 1 + 2
    pl.semaphore_wait(barrier, peers)

    def spectrum_copy(piece, shift):
        target = lax.rem(band + shift, bands)
        at = piece * bands + shift
        return pltpu.make_async_remote_copy(
            src_ref=send_buf.at[target, piece],
            dst_ref=recv_buf.at[piece, band],
            send_sem=a_send.at[at],
            recv_sem=a_recv.at[at],
            device_id={"band": target},
            device_id_type=MESH,
        )

    spectrum_copies = [[spectrum_copy(piece, shift) for shift in range(1, bands)] for piece in range(pieces)]
    for piece in range(pieces):
        for copy in spectrum_copies[piece]:
            copy.start()

    weights, offsets = ([], [])
    for k in range(count):
        weights.append(table_ref[index_ref[k]])
        position = (chan * count + k).astype(jnp.float32)
        offsets.append((2.0 * position + 1.0) / (count * groups) - 1.0)
    coeffs = [weights, [w * o for w, o in zip(weights, offsets)], [w * o * o for w, o in zip(weights, offsets)]]
    powers = list(weights)
    moments = []
    for power in range(5):
        total = powers[0]
        for k in range(1, count):
            total = total + powers[k]
        moments.append(total)
        powers = [p * o for p, o in zip(powers, offsets)]
    sublane = lax.broadcasted_iota(jnp.int32, (8, 128), 0)
    moment_tile = jnp.zeros((8, 128), jnp.float32)
    for power in range(5):
        moment_tile = jnp.where(sublane == power, moments[power], moment_tile)

    def sums(k, target_ref, slot, extra):
        res_copies[k].wait()

        def tile(step, carry):
            row = step // lane_tiles
            lane = lax.rem(step, lane_tiles)
            rows_at = pl.ds(pl.multiple_of(row * 8, 8), 8)
            lanes_at = pl.ds(pl.multiple_of(lane * 128, 128), 128)
            totals = [None] * TERMS
            for channel in range(count):
                value = res_buf[k, channel, rows_at, lanes_at]
                for term in range(TERMS):
                    product = value * coeffs[term][channel]
                    totals[term] = product if totals[term] is None else totals[term] + product
            for term in range(TERMS):
                at = term * plane + step
                total = totals[term]
                if extra is not None:
                    total = total + extra[slot, at]
                target_ref[slot, at] = total
            return carry

        lax.fori_loop(0, plane, tile, 0, unroll=4)
        moment = moment_tile
        if extra is not None:
            moment = moment + extra[slot, TERMS * plane]
        target_ref[slot, TERMS * plane] = moment

    core_copies = []
    for slot in range(len(slots)):
        sums(slot, core_send, slot, None)
        copy = pltpu.make_async_remote_copy(
            src_ref=core_send.at[slot],
            dst_ref=core_recv.at[slot],
            send_sem=c_send.at[slot],
            recv_sem=c_recv.at[slot],
            device_id=partner,
            device_id_type=MESH,
        )
        copy.start()
        core_copies.append(copy)

    z_copies = {}
    for slot, (other, shift) in enumerate(slots):
        core_copies[slot].wait_recv()
        sums(len(slots) + slot, own_buf, slot, core_recv)
        if shift:
            copy = pltpu.make_async_remote_copy(
                src_ref=own_buf.at[slot],
                dst_ref=z_recv.at[slot],
                send_sem=z_send_sem.at[slot],
                recv_sem=z_recv_sem.at[slot],
                device_id={"chan": chan_of(x_lo, z_of(shift), core)},
                device_id_type=MESH,
            )
            copy.start()
            z_copies[slot] = copy

    own = send_buf.at[band]
    for piece in range(pieces):
        recv_buf[piece, band] = own[piece]

    def gathered(other, target):
        base = [k for k, key in enumerate(slots) if key == (other, 0)][0]
        came = [k for k, key in enumerate(slots) if key[0] == other and key[1]]
        for slot in came:
            z_copies[slot].wait_recv()

        def tile(step, carry):
            total = own_buf[base, step]
            for slot in came:
                total = total + z_recv[slot, step]
            target[step] = total
            return carry

        lax.fori_loop(0, TERMS * plane + 1, tile, 0)

    gathered(1, x_send)
    x_copy = pltpu.make_async_remote_copy(
        src_ref=x_send,
        dst_ref=x_recv,
        send_sem=x_send_sem,
        recv_sem=x_recv_sem,
        device_id=across,
        device_id_type=MESH,
    )
    x_copy.start()

    def place(piece):
        half, part = divmod(piece, 2)
        for copy in spectrum_copies[piece]:
            copy.wait_recv()

        def turn(k, carry):
            for side in range(2):
                value = jnp.concatenate(
                    [recv_buf[piece, side * 4 + source, pl.ds(k, 32, stride=8), :] for source in range(4)],
                    axis=0,
                )
                start = pl.multiple_of((half * 8 + k) * RADIX, RADIX)
                spec_ref[part, pl.ds(start, RADIX), pl.ds(side * 128, 128)] = value.T
            return carry

        lax.fori_loop(0, 8, turn, 0)

    def finish():
        gathered(0, own_buf.at[len(slots) - 1])
        x_copy.wait_recv()
        last = len(slots) - 1
        total = own_buf[last, TERMS * plane] + x_recv[TERMS * plane]
        inverse = solve_rows([total[k : k + 1] for k in range(5)], None)

        def tile(step, carry):
            row = step // lane_tiles
            lane = lax.rem(step, lane_tiles)
            rows_at = pl.ds(pl.multiple_of(row * 8, 8), 8)
            lanes_at = pl.ds(pl.multiple_of(lane * 128, 128), 128)
            taylor = [own_buf[last, s * plane + step] + x_recv[s * plane + step] for s in range(TERMS)]
            for t in range(TERMS):
                comp_ref[t, rows_at, lanes_at] = (
                    inverse[t][0] * taylor[0] + inverse[t][1] * taylor[1] + inverse[t][2] * taylor[2]
                )
            return carry

        lax.fori_loop(0, plane, tile, 0)

    for piece in range(pieces):
        place(piece)
    finish()

    for piece in range(pieces):
        for copy in spectrum_copies[piece]:
            copy.wait_send()
    for copy in core_copies:
        copy.wait_send()
    for copy in z_copies.values():
        copy.wait_send()
    x_copy.wait_send()


def write_out(comp_ref, spec_ref, comp_hbm, spec_hbm, sem):
    copies = [pltpu.make_async_copy(comp_ref, comp_hbm, sem.at[0])]
    copies += [pltpu.make_async_copy(spec_ref.at[part], spec_hbm.at[part], sem.at[1 + part]) for part in range(2)]
    for copy in copies:
        copy.start()
    for copy in copies:
        copy.wait()


def local(residual, weight_index, weight_table, gridded):
    bands = lax.axis_size("band")
    groups = lax.axis_size("chan")
    count, rows, width = residual.shape
    grid_rows, length = gridded.shape[2:]
    blocks = grid_rows // 8
    tiled = gridded.reshape(2, blocks, 8, RADIX, RADIX)
    tiled = jnp.transpose(tiled, (0, 1, 3, 2, 4)).reshape(2, blocks, RADIX * 8, RADIX)
    columns = width // groups
    out_length = length // bands
    pieces = 2 * (RADIX // bands // 8)
    tiles = TERMS * (rows // 8) * (columns // 128) + 1
    f32 = jnp.float32
    any_space = pl.BlockSpec(memory_space=pl.ANY)
    vmem = pl.BlockSpec(memory_space=pltpu.VMEM)
    dma = pltpu.SemaphoreType.DMA
    slots = 2 * len(SHIFTS)
    components, spectrum = pl.pallas_call(
        body,
        out_shape=(
            pltpu.VMEM((TERMS, rows, columns), f32),
            pltpu.VMEM((2, out_length, grid_rows * bands), f32),
        ),
        in_specs=[any_space] * 6,
        out_specs=(vmem, vmem),
        scratch_shapes=[
            pltpu.SMEM(weight_index.shape, weight_index.dtype),
            pltpu.SMEM(weight_table.shape, f32),
            pltpu.VMEM((4 * RADIX, 2 * RADIX), jnp.bfloat16),
            pltpu.VMEM((2, RADIX, RADIX), f32),
            pltpu.VMEM((2, blocks, RADIX * 8, RADIX), f32),
            pltpu.VMEM((groups, count, rows, columns), f32),
            pltpu.VMEM((bands, pieces, grid_rows * 8, RADIX), f32),
            pltpu.VMEM((pieces, bands, grid_rows * 8, RADIX), f32),
            pltpu.VMEM((slots, tiles, 8, 128), f32),
            pltpu.VMEM((slots, tiles, 8, 128), f32),
            pltpu.VMEM((slots, tiles, 8, 128), f32),
            pltpu.VMEM((slots, tiles, 8, 128), f32),
            pltpu.VMEM((tiles, 8, 128), f32),
            pltpu.VMEM((tiles, 8, 128), f32),
            dma((4,)),
            dma((blocks,)),
            dma((groups,)),
            dma((pieces * bands,)),
            dma((pieces * bands,)),
            dma((slots,)),
            dma((slots,)),
            dma((slots,)),
            dma((slots,)),
            dma,
            dma,
        ],
        compiler_params=pltpu.CompilerParams(
            collective_id=0, has_side_effects=True, vmem_limit_bytes=52 << 20
        ),
    )(residual, weight_index, weight_table, tiled, *(jnp.asarray(table) for table in tables()))
    components, spectrum = pl.pallas_call(
        write_out,
        out_shape=(
            jax.ShapeDtypeStruct(components.shape, f32),
            jax.ShapeDtypeStruct(spectrum.shape, f32),
        ),
        in_specs=[vmem, vmem],
        out_specs=(any_space, any_space),
        scratch_shapes=[dma((3,))],
        compiler_params=pltpu.CompilerParams(vmem_limit_bytes=6 << 20),
    )(*(pltpu.with_memory_space_constraint(array, pltpu.VMEM) for array in (components, spectrum)))
    return (components, spectrum.reshape(2, 1, out_length, grid_rows * bands))


def solution(mesh):
    in_specs = (P("chan", "band", None), P("chan"), P(), P(None, "chan", "band", None))
    out_specs = (P(None, "band", "chan"), P(None, "chan", "band", None))
    return jax.shard_map(local, mesh=mesh, in_specs=in_specs, out_specs=out_specs, check_vma=False)
```

```python
import functools

import jax
import jax.numpy as jnp
import numpy as np
from jax import lax
from jax.experimental import pallas as pl
from jax.experimental.pallas import tpu as pltpu
from jax.sharding import PartitionSpec as P

MESH = pl.DeviceIdType.MESH
RADIX = 128
TERMS = 3
SHIFTS = (2, 1, 3, 0)
READY = 1


def tables():
    step = np.arange(RADIX)
    angle = 2.0 * np.pi * (np.outer(step, step) % RADIX) / RADIX
    cos, sin = (np.cos(angle), np.sin(angle))
    whole = np.block([[cos, sin], [-sin, cos]]).astype(np.float32)
    high = whole.astype(jnp.bfloat16)
    low = (whole - high.astype(np.float32)).astype(jnp.bfloat16)
    turn = 2.0 * np.pi * np.outer(step, step) / (RADIX * RADIX)
    twist = np.stack([np.cos(turn), -np.sin(turn)]) / RADIX
    return (np.concatenate([high, low]), twist.astype(np.float32))


def three_products(pair, value, axis):
    width = 2 * RADIX
    mul = functools.partial(
        lax.dot_general,
        dimension_numbers=(((1,), (axis,)), ((), ())),
        preferred_element_type=jnp.float32,
    )
    done = []
    for k in range(value.shape[1 - axis] // width):
        cut = slice(k * width, (k + 1) * width)
        tile = value[:, cut] if axis == 0 else value[cut]
        high = tile.astype(jnp.bfloat16)
        low = (tile - high.astype(jnp.float32)).astype(jnp.bfloat16)
        both = mul(pair, high)
        done.append(both[:width] + (both[width:] + mul(pair[:width], low)))
    return jnp.concatenate(done, axis=1)


def solve_rows(moment, taylor):
    m0, m1, m2, m3, m4 = moment
    aa = m2 * m4 - m3 * m3
    ab = m2 * m3 - m1 * m4
    ac = m1 * m3 - m2 * m2
    bb = m0 * m4 - m2 * m2
    bc = m1 * m2 - m0 * m3
    cc = m0 * m2 - m1 * m1
    determ = m0 * aa + m1 * ab + m2 * ac
    aa, ab, ac, bb, bc, cc = (entry / determ for entry in (aa, ab, ac, bb, bc, cc))
    return ((aa, ab, ac), (ab, bb, bc), (ac, bc, cc))


def body(
    res_hbm, index_hbm, table_hbm, grid_hbm, pair_hbm, twist_hbm,
    comp_ref, spec_ref,
    index_ref, table_ref, pair_ref, twist_ref, grid_buf, res_buf, send_buf, recv_buf, core_send, own_buf, core_recv, z_recv, x_send, x_recv,
    small_sem, grid_sem, res_sem, a_send, a_recv, c_send, c_recv, z_send_sem, z_recv_sem, x_send_sem, x_recv_sem,
):
    groups = lax.axis_size("chan")
    bands = lax.axis_size("band")
    zs = groups // 4
    chan = lax.axis_index("chan")
    band = lax.axis_index("band")
    x_lo = chan // (2 * zs)
    z_at = (chan // 2) % zs
    core = chan % 2
    count = res_hbm.shape[0]
    rows = res_hbm.shape[1]
    columns = res_hbm.shape[2] // groups
    row_tiles = rows // 8
    lane_tiles = columns // 128
    plane = row_tiles * lane_tiles
    blocks = grid_hbm.shape[1]
    halves = send_buf.shape[2] // 2

    def chan_of(x, z, c):
        return (x * zs + z) * 2 + c

    def z_of(shift):
        return lax.rem(z_at + shift, zs)

    partner = {"chan": chan_of(x_lo, z_at, 1 - core)}
    across = {"chan": chan_of(1 - x_lo, z_at, core)}

    barrier = pltpu.get_barrier_semaphore()
    for shift in range(1, bands):
        pl.semaphore_signal(barrier, 1, device_id={"band": lax.rem(band + shift, bands)}, device_id_type=MESH)
    for shift in SHIFTS[:-1]:
        pl.semaphore_signal(barrier, 1, device_id={"chan": chan_of(x_lo, z_of(shift), core)}, device_id_type=MESH)
    pl.semaphore_signal(barrier, 1, device_id=partner, device_id_type=MESH)
    pl.semaphore_signal(barrier, 1, device_id=across, device_id_type=MESH)

    grid_copies = [
        pltpu.make_async_copy(grid_hbm.at[:, k], grid_buf.at[:, k], grid_sem.at[k]) for k in range(blocks)
    ]
    small_copies = [
        pltpu.make_async_copy(source, target, small_sem.at[k])
        for k, (source, target) in enumerate(
            ((pair_hbm, pair_ref), (twist_hbm, twist_ref), (index_hbm, index_ref), (table_hbm, table_ref))
        )
    ]
    for copy in (grid_copies[0], *small_copies, *grid_copies[1:]):
        copy.start()
    slots = [(other, shift) for other in (1, 0) for shift in SHIFTS]
    order = [(away, slot) for away in (1, 0) for slot in range(len(slots))]

    def block_of(away, slot):
        other, shift = slots[slot]
        return chan_of((x_lo + other) % 2, z_of(shift), (core + away) % 2)

    res_copies = []
    for k, (away, slot) in enumerate(order):
        start = pl.multiple_of(block_of(away, slot) * columns, columns)
        res_copies.append(
            pltpu.make_async_copy(res_hbm.at[:, :, pl.ds(start, columns)], res_buf.at[k], res_sem.at[k])
        )

    for copy in small_copies:
        copy.wait()

    def transform(block):
        def taken(part):
            return jnp.concatenate([grid_buf[part, block, pl.ds(k, RADIX, stride=8), :] for k in range(8)], axis=1)

        pair = pair_ref[...]
        stage = three_products(pair, jnp.concatenate([taken(0), taken(1)], axis=0), 0)
        tre, tim = (twist_ref[0], twist_ref[1])
        turned = []
        for k in range(8):
            cut = slice(k * RADIX, (k + 1) * RADIX)
            real, imag = (stage[:RADIX, cut], stage[RADIX:, cut])
            turned.append(jnp.concatenate([real * tre - imag * tim, real * tim + imag * tre], axis=1))
        final = three_products(pair, jnp.concatenate(turned, axis=0), 1)
        for k in range(8):
            for target in range(bands):
                for part in range(2):
                    for half in range(halves):
                        at = part * RADIX + target * (8 * halves) + half * 8
                        send_buf[target, block, half * 2 + part, k * 8 : k * 8 + 8, :] = final[
                            at : at + 8, k * RADIX : (k + 1) * RADIX
                        ]

    def spectrum_copy(piece, shift):
        target = lax.rem(band + shift, bands)
        at = piece * bands + shift
        return pltpu.make_async_remote_copy(
            src_ref=send_buf.at[target, piece],
            dst_ref=recv_buf.at[piece, band],
            send_sem=a_send.at[at],
            recv_sem=a_recv.at[at],
            device_id={"band": target},
            device_id_type=MESH,
        )

    spectrum_copies = [[spectrum_copy(piece, shift) for shift in range(1, bands)] for piece in range(blocks)]
    peers = bands - 1 + len(SHIFTS) - 1 + 2
    for block in range(blocks):
        grid_copies[block].wait()
        if block == blocks - 1:
            for copy in res_copies:
                copy.start()
        transform(block)
        if block == READY:
            pl.semaphore_wait(barrier, peers)
            for piece in range(READY):
                for copy in spectrum_copies[piece]:
                    copy.start()
        if block >= READY:
            for copy in spectrum_copies[block]:
                copy.start()

    weights, offsets = ([], [])
    for k in range(count):
        weights.append(table_ref[index_ref[k]])
        position = (chan * count + k).astype(jnp.float32)
        offsets.append((2.0 * position + 1.0) / (count * groups) - 1.0)
    coeffs = [weights, [w * o for w, o in zip(weights, offsets)], [w * o * o for w, o in zip(weights, offsets)]]
    powers = list(weights)
    moments = []
    for power in range(5):
        total = powers[0]
        for k in range(1, count):
            total = total + powers[k]
        moments.append(total)
        powers = [p * o for p, o in zip(powers, offsets)]
    sublane = lax.broadcasted_iota(jnp.int32, (8, 128), 0)
    moment_tile = jnp.zeros((8, 128), jnp.float32)
    for power in range(5):
        moment_tile = jnp.where(sublane == power, moments[power], moment_tile)

    def sums(k, target_ref, slot, extra):
        res_copies[k].wait()

        def tile(step, carry):
            row = step // lane_tiles
            lane = lax.rem(step, lane_tiles)
            rows_at = pl.ds(pl.multiple_of(row * 8, 8), 8)
            lanes_at = pl.ds(pl.multiple_of(lane * 128, 128), 128)
            totals = [None] * TERMS
            for channel in range(count):
                value = res_buf[k, channel, rows_at, lanes_at]
                for term in range(TERMS):
                    product = value * coeffs[term][channel]
                    totals[term] = product if totals[term] is None else totals[term] + product
            for term in range(TERMS):
                at = term * plane + step
                total = totals[term]
                if extra is not None:
                    total = total + extra[slot, at]
                target_ref[slot, at] = total
            return carry

        lax.fori_loop(0, plane, tile, 0, unroll=4)
        moment = moment_tile
        if extra is not None:
            moment = moment + extra[slot, TERMS * plane]
        target_ref[slot, TERMS * plane] = moment

    core_copies = []
    for slot in range(len(slots)):
        sums(slot, core_send, slot, None)
        copy = pltpu.make_async_remote_copy(
            src_ref=core_send.at[slot],
            dst_ref=core_recv.at[slot],
            send_sem=c_send.at[slot],
            recv_sem=c_recv.at[slot],
            device_id=partner,
            device_id_type=MESH,
        )
        copy.start()
        core_copies.append(copy)

    z_copies = {}
    for slot, (other, shift) in enumerate(slots):
        core_copies[slot].wait_recv()
        sums(len(slots) + slot, own_buf, slot, core_recv)
        if shift:
            copy = pltpu.make_async_remote_copy(
                src_ref=own_buf.at[slot],
                dst_ref=z_recv.at[slot],
                send_sem=z_send_sem.at[slot],
                recv_sem=z_recv_sem.at[slot],
                device_id={"chan": chan_of(x_lo, z_of(shift), core)},
                device_id_type=MESH,
            )
            copy.start()
            z_copies[slot] = copy

    own = send_buf.at[band]
    for piece in range(blocks):
        recv_buf[piece, band] = own[piece]

    def gathered(other, target):
        base = [k for k, key in enumerate(slots) if key == (other, 0)][0]
        came = [k for k, key in enumerate(slots) if key[0] == other and key[1]]
        for slot in came:
            z_copies[slot].wait_recv()

        def tile(step, carry):
            total = own_buf[base, step]
            for slot in came:
                total = total + z_recv[slot, step]
            target[step] = total
            return carry

        lax.fori_loop(0, TERMS * plane + 1, tile, 0)

    gathered(1, x_send)
    x_copy = pltpu.make_async_remote_copy(
        src_ref=x_send,
        dst_ref=x_recv,
        send_sem=x_send_sem,
        recv_sem=x_recv_sem,
        device_id=across,
        device_id_type=MESH,
    )
    x_copy.start()

    def place(half, part):
        def turn(k, carry):
            for side in range(2):
                value = jnp.concatenate(
                    [
                        recv_buf[piece, side * 4 + source, half * 2 + part, pl.ds(k, 8, stride=8), :]
                        for source in range(4)
                        for piece in range(blocks)
                    ],
                    axis=0,
                )
                start = pl.multiple_of((half * 8 + k) * RADIX, RADIX)
                spec_ref[part, pl.ds(start, RADIX), pl.ds(side * 128, 128)] = value.T
            return carry

        lax.fori_loop(0, 8, turn, 0)

    def finish():
        gathered(0, own_buf.at[len(slots) - 1])
        x_copy.wait_recv()
        last = len(slots) - 1
        total = own_buf[last, TERMS * plane] + x_recv[TERMS * plane]
        inverse = solve_rows([total[k : k + 1] for k in range(5)], None)

        def tile(step, carry):
            row = step // lane_tiles
            lane = lax.rem(step, lane_tiles)
            rows_at = pl.ds(pl.multiple_of(row * 8, 8), 8)
            lanes_at = pl.ds(pl.multiple_of(lane * 128, 128), 128)
            taylor = [own_buf[last, s * plane + step] + x_recv[s * plane + step] for s in range(TERMS)]
            for t in range(TERMS):
                comp_ref[t, rows_at, lanes_at] = (
                    inverse[t][0] * taylor[0] + inverse[t][1] * taylor[1] + inverse[t][2] * taylor[2]
                )
            return carry

        lax.fori_loop(0, plane, tile, 0)

    for copies in spectrum_copies:
        for copy in copies:
            copy.wait_recv()
    for half in range(halves):
        for part in range(2):
            place(half, part)
    finish()

    for copies in spectrum_copies:
        for copy in copies:
            copy.wait_send()
    for copy in core_copies:
        copy.wait_send()
    for copy in z_copies.values():
        copy.wait_send()
    x_copy.wait_send()


def write_out(comp_ref, spec_ref, comp_hbm, spec_hbm, sem):
    copies = [pltpu.make_async_copy(comp_ref, comp_hbm, sem.at[0])]
    copies += [pltpu.make_async_copy(spec_ref.at[part], spec_hbm.at[part], sem.at[1 + part]) for part in range(2)]
    for copy in copies:
        copy.start()
    for copy in copies:
        copy.wait()


def local(residual, weight_index, weight_table, gridded):
    bands = lax.axis_size("band")
    groups = lax.axis_size("chan")
    count, rows, width = residual.shape
    grid_rows, length = gridded.shape[2:]
    blocks = grid_rows // 8
    tiled = gridded.reshape(2, blocks, 8, RADIX, RADIX)
    tiled = jnp.transpose(tiled, (0, 1, 3, 2, 4)).reshape(2, blocks, RADIX * 8, RADIX)
    columns = width // groups
    out_length = length // bands
    quarters = 2 * (RADIX // bands // 8)
    tiles = TERMS * (rows // 8) * (columns // 128) + 1
    f32 = jnp.float32
    any_space = pl.BlockSpec(memory_space=pl.ANY)
    vmem = pl.BlockSpec(memory_space=pltpu.VMEM)
    dma = pltpu.SemaphoreType.DMA
    slots = 2 * len(SHIFTS)
    components, spectrum = pl.pallas_call(
        body,
        out_shape=(
            pltpu.VMEM((TERMS, rows, columns), f32),
            pltpu.VMEM((2, out_length, grid_rows * bands), f32),
        ),
        in_specs=[any_space] * 6,
        out_specs=(vmem, vmem),
        scratch_shapes=[
            pltpu.SMEM(weight_index.shape, weight_index.dtype),
            pltpu.SMEM(weight_table.shape, f32),
            pltpu.VMEM((4 * RADIX, 2 * RADIX), jnp.bfloat16),
            pltpu.VMEM((2, RADIX, RADIX), f32),
            pltpu.VMEM((2, blocks, RADIX * 8, RADIX), f32),
            pltpu.VMEM((groups, count, rows, columns), f32),
            pltpu.VMEM((bands, blocks, quarters, 64, RADIX), f32),
            pltpu.VMEM((blocks, bands, quarters, 64, RADIX), f32),
            pltpu.VMEM((slots, tiles, 8, 128), f32),
            pltpu.VMEM((slots, tiles, 8, 128), f32),
            pltpu.VMEM((slots, tiles, 8, 128), f32),
            pltpu.VMEM((slots, tiles, 8, 128), f32),
            pltpu.VMEM((tiles, 8, 128), f32),
            pltpu.VMEM((tiles, 8, 128), f32),
            dma((4,)),
            dma((blocks,)),
            dma((groups,)),
            dma((blocks * bands,)),
            dma((blocks * bands,)),
            dma((slots,)),
            dma((slots,)),
            dma((slots,)),
            dma((slots,)),
            dma,
            dma,
        ],
        compiler_params=pltpu.CompilerParams(
            collective_id=0, has_side_effects=True, vmem_limit_bytes=52 << 20
        ),
    )(residual, weight_index, weight_table, tiled, *(jnp.asarray(table) for table in tables()))
    components, spectrum = pl.pallas_call(
        write_out,
        out_shape=(
            jax.ShapeDtypeStruct(components.shape, f32),
            jax.ShapeDtypeStruct(spectrum.shape, f32),
        ),
        in_specs=[vmem, vmem],
        out_specs=(any_space, any_space),
        scratch_shapes=[dma((3,))],
        compiler_params=pltpu.CompilerParams(vmem_limit_bytes=6 << 20),
    )(*(pltpu.with_memory_space_constraint(array, pltpu.VMEM) for array in (components, spectrum)))
    return (components, spectrum.reshape(2, 1, out_length, grid_rows * bands))


def solution(mesh):
    in_specs = (P("chan", "band", None), P("chan"), P(), P(None, "chan", "band", None))
    out_specs = (P(None, "band", "chan"), P(None, "chan", "band", None))
    return jax.shard_map(local, mesh=mesh, in_specs=in_specs, out_specs=out_specs, check_vma=False)
```

```python
import functools

import jax
import jax.numpy as jnp
import numpy as np
from jax import lax
from jax.experimental import pallas as pl
from jax.experimental.pallas import tpu as pltpu
from jax.sharding import PartitionSpec as P

MESH = pl.DeviceIdType.MESH
RADIX = 128
TERMS = 3
SHIFTS = (2, 1, 3, 0)
READY = 1
FAR = 2


def tables():
    step = np.arange(RADIX)
    angle = 2.0 * np.pi * (np.outer(step, step) % RADIX) / RADIX
    cos, sin = (np.cos(angle), np.sin(angle))
    whole = np.block([[cos, sin], [-sin, cos]]).astype(np.float32)
    high = whole.astype(jnp.bfloat16)
    low = (whole - high.astype(np.float32)).astype(jnp.bfloat16)
    turn = 2.0 * np.pi * np.outer(step, step) / (RADIX * RADIX)
    twist = np.stack([np.cos(turn), -np.sin(turn)]) / RADIX
    return (np.concatenate([high, low]), twist.astype(np.float32))


def three_products(pair, value, axis):
    width = 2 * RADIX
    mul = functools.partial(
        lax.dot_general,
        dimension_numbers=(((1,), (axis,)), ((), ())),
        preferred_element_type=jnp.float32,
    )
    done = []
    for k in range(value.shape[1 - axis] // width):
        cut = slice(k * width, (k + 1) * width)
        tile = value[:, cut] if axis == 0 else value[cut]
        high = tile.astype(jnp.bfloat16)
        low = (tile - high.astype(jnp.float32)).astype(jnp.bfloat16)
        both = mul(pair, high)
        done.append(both[:width] + (both[width:] + mul(pair[:width], low)))
    return jnp.concatenate(done, axis=1)


def solve_rows(moment, taylor):
    m0, m1, m2, m3, m4 = moment
    aa = m2 * m4 - m3 * m3
    ab = m2 * m3 - m1 * m4
    ac = m1 * m3 - m2 * m2
    bb = m0 * m4 - m2 * m2
    bc = m1 * m2 - m0 * m3
    cc = m0 * m2 - m1 * m1
    determ = m0 * aa + m1 * ab + m2 * ac
    aa, ab, ac, bb, bc, cc = (entry / determ for entry in (aa, ab, ac, bb, bc, cc))
    return ((aa, ab, ac), (ab, bb, bc), (ac, bc, cc))


def body(
    res_hbm, index_hbm, table_hbm, grid_hbm, pair_hbm, twist_hbm,
    comp_ref, spec_ref,
    index_ref, table_ref, pair_ref, twist_ref, grid_buf, res_buf, send_buf, recv_buf, core_send, own_buf, core_recv, z_recv, x_send, x_recv,
    word_sem, small_sem, grid_sem, res_sem, a_send, a_recv, c_send, c_recv, z_send_sem, z_recv_sem, x_send_sem, x_recv_sem,
):
    groups = lax.axis_size("chan")
    bands = lax.axis_size("band")
    zs = groups // 4
    chan = lax.axis_index("chan")
    band = lax.axis_index("band")
    x_lo = chan // (2 * zs)
    z_at = (chan // 2) % zs
    core = chan % 2
    ys = bands // 2
    y_at = band // 2
    x_hi = band % 2
    count = res_hbm.shape[0]
    rows = res_hbm.shape[1]
    columns = res_hbm.shape[2] // groups
    row_tiles = rows // 8
    lane_tiles = columns // 128
    plane = row_tiles * lane_tiles
    blocks = grid_hbm.shape[1]
    halves = send_buf.shape[2] // 2

    def chan_of(x, z, c):
        return (x * zs + z) * 2 + c

    def z_of(shift):
        return lax.rem(z_at + shift, zs)

    partner = {"chan": chan_of(x_lo, z_at, 1 - core)}
    across = {"chan": chan_of(1 - x_lo, z_at, core)}

    def along(turn):
        return {"band": lax.rem(y_at + turn, ys) * 2 + x_hi}

    def beyond(turn):
        return {"band": lax.rem(y_at + turn, ys) * 2 + 1 - x_hi}

    def up(turn):
        return {"chan": chan_of(x_lo, z_of(turn), core)}

    nearest = (beyond(0), along(1), along(ys - 1), up(1), up(zs - 1), partner, across)
    barrier = pltpu.get_barrier_semaphore()
    for device in nearest:
        pl.semaphore_signal(barrier, 1, device_id=device, device_id_type=MESH)

    grid_copies = [
        pltpu.make_async_copy(grid_hbm.at[:, k], grid_buf.at[:, k], grid_sem.at[k]) for k in range(blocks)
    ]
    small_copies = [
        pltpu.make_async_copy(source, target, small_sem.at[k])
        for k, (source, target) in enumerate(
            ((pair_hbm, pair_ref), (twist_hbm, twist_ref), (index_hbm, index_ref), (table_hbm, table_ref))
        )
    ]
    for copy in (grid_copies[0], *small_copies, *grid_copies[1:]):
        copy.start()
    slots = [(other, shift) for other in (1, 0) for shift in SHIFTS]
    order = [(away, slot) for away in (1, 0) for slot in range(len(slots))]

    def block_of(away, slot):
        other, shift = slots[slot]
        return chan_of((x_lo + other) % 2, z_of(shift), (core + away) % 2)

    res_copies = []
    for k, (away, slot) in enumerate(order):
        start = pl.multiple_of(block_of(away, slot) * columns, columns)
        res_copies.append(
            pltpu.make_async_copy(res_hbm.at[:, :, pl.ds(start, columns)], res_buf.at[k], res_sem.at[k])
        )

    for copy in small_copies:
        copy.wait()

    def transform(block):
        def taken(part):
            return jnp.concatenate([grid_buf[part, block, pl.ds(k, RADIX, stride=8), :] for k in range(8)], axis=1)

        pair = pair_ref[...]
        stage = three_products(pair, jnp.concatenate([taken(0), taken(1)], axis=0), 0)
        tre, tim = (twist_ref[0], twist_ref[1])
        turned = []
        for k in range(8):
            cut = slice(k * RADIX, (k + 1) * RADIX)
            real, imag = (stage[:RADIX, cut], stage[RADIX:, cut])
            turned.append(jnp.concatenate([real * tre - imag * tim, real * tim + imag * tre], axis=1))
        final = three_products(pair, jnp.concatenate(turned, axis=0), 1)
        for k in range(8):
            for target in range(bands):
                for part in range(2):
                    for half in range(halves):
                        at = part * RADIX + target * (8 * halves) + half * 8
                        send_buf[target, block, half * 2 + part, k * 8 : k * 8 + 8, :] = final[
                            at : at + 8, k * RADIX : (k + 1) * RADIX
                        ]

    def spectrum_copy(piece, crossing, turn):
        device = beyond(turn) if crossing else along(turn)
        at = piece * bands + turn * 2 + crossing
        return pltpu.make_async_remote_copy(
            src_ref=send_buf.at[device["band"], piece],
            dst_ref=recv_buf.at[piece, band],
            send_sem=a_send.at[at],
            recv_sem=a_recv.at[at],
            device_id=device,
            device_id_type=MESH,
        )

    ways = [(1, 2), (1, 1), (1, ys - 1), (0, 2), (1, 0), (0, 1), (0, ys - 1)]
    spectrum_copies = [[spectrum_copy(piece, *way) for way in ways] for piece in range(blocks)]

    def started(pieces, chosen):
        for piece in pieces:
            for way in chosen:
                spectrum_copies[piece][way].start()

    for block in range(blocks):
        grid_copies[block].wait()
        if block == blocks - 1:
            for copy in res_copies:
                copy.start()
        transform(block)
        if block == READY:
            pl.semaphore_wait(barrier, len(nearest))
            pl.semaphore_signal(word_sem.at[0], 1, device_id=beyond(0), device_id_type=MESH)
            pl.semaphore_signal(word_sem.at[1], 1, device_id=along(ys - 1), device_id_type=MESH)
            pl.semaphore_signal(word_sem.at[2], 1, device_id=up(zs - 1), device_id_type=MESH)
            started(range(READY + 1), (4,))
            started((0,), (5, 6))
        if block == FAR:
            pl.semaphore_wait(word_sem.at[1], 1)
            pl.semaphore_signal(word_sem.at[3], 1, device_id=beyond(0), device_id_type=MESH)
            pl.semaphore_wait(word_sem.at[0], 1)
            started((0,), (1, 2, 3))
            started(range(1, READY + 1), (1, 2, 3, 5, 6))
        if block == blocks - 1:
            pl.semaphore_wait(word_sem.at[3], 1)
            pl.semaphore_wait(word_sem.at[2], 1)
            started(range(READY + 1), (0,))
            started(range(READY + 1, blocks), range(7))

    weights, offsets = ([], [])
    for k in range(count):
        weights.append(table_ref[index_ref[k]])
        position = (chan * count + k).astype(jnp.float32)
        offsets.append((2.0 * position + 1.0) / (count * groups) - 1.0)
    coeffs = [weights, [w * o for w, o in zip(weights, offsets)], [w * o * o for w, o in zip(weights, offsets)]]
    powers = list(weights)
    moments = []
    for power in range(5):
        total = powers[0]
        for k in range(1, count):
            total = total + powers[k]
        moments.append(total)
        powers = [p * o for p, o in zip(powers, offsets)]
    sublane = lax.broadcasted_iota(jnp.int32, (8, 128), 0)
    moment_tile = jnp.zeros((8, 128), jnp.float32)
    for power in range(5):
        moment_tile = jnp.where(sublane == power, moments[power], moment_tile)

    def sums(k, target_ref, slot, extra):
        res_copies[k].wait()

        def tile(step, carry):
            row = step // lane_tiles
            lane = lax.rem(step, lane_tiles)
            rows_at = pl.ds(pl.multiple_of(row * 8, 8), 8)
            lanes_at = pl.ds(pl.multiple_of(lane * 128, 128), 128)
            totals = [None] * TERMS
            for channel in range(count):
                value = res_buf[k, channel, rows_at, lanes_at]
                for term in range(TERMS):
                    product = value * coeffs[term][channel]
                    totals[term] = product if totals[term] is None else totals[term] + product
            for term in range(TERMS):
                at = term * plane + step
                total = totals[term]
                if extra is not None:
                    total = total + extra[slot, at]
                target_ref[slot, at] = total
            return carry

        lax.fori_loop(0, plane, tile, 0, unroll=4)
        moment = moment_tile
        if extra is not None:
            moment = moment + extra[slot, TERMS * plane]
        target_ref[slot, TERMS * plane] = moment

    core_copies = []
    for slot in range(len(slots)):
        sums(slot, core_send, slot, None)
        copy = pltpu.make_async_remote_copy(
            src_ref=core_send.at[slot],
            dst_ref=core_recv.at[slot],
            send_sem=c_send.at[slot],
            recv_sem=c_recv.at[slot],
            device_id=partner,
            device_id_type=MESH,
        )
        copy.start()
        core_copies.append(copy)

    z_copies = {}
    for slot, (other, shift) in enumerate(slots):
        core_copies[slot].wait_recv()
        sums(len(slots) + slot, own_buf, slot, core_recv)
        if shift:
            copy = pltpu.make_async_remote_copy(
                src_ref=own_buf.at[slot],
                dst_ref=z_recv.at[slot],
                send_sem=z_send_sem.at[slot],
                recv_sem=z_recv_sem.at[slot],
                device_id={"chan": chan_of(x_lo, z_of(shift), core)},
                device_id_type=MESH,
            )
            copy.start()
            z_copies[slot] = copy

    own = send_buf.at[band]
    for piece in range(blocks):
        recv_buf[piece, band] = own[piece]

    def gathered(other, target):
        base = [k for k, key in enumerate(slots) if key == (other, 0)][0]
        came = [k for k, key in enumerate(slots) if key[0] == other and key[1]]
        for slot in came:
            z_copies[slot].wait_recv()

        def tile(step, carry):
            total = own_buf[base, step]
            for slot in came:
                total = total + z_recv[slot, step]
            target[step] = total
            return carry

        lax.fori_loop(0, TERMS * plane + 1, tile, 0)

    gathered(1, x_send)
    x_copy = pltpu.make_async_remote_copy(
        src_ref=x_send,
        dst_ref=x_recv,
        send_sem=x_send_sem,
        recv_sem=x_recv_sem,
        device_id=across,
        device_id_type=MESH,
    )
    x_copy.start()

    def place(half, part):
        def turn(k, carry):
            for side in range(2):
                value = jnp.concatenate(
                    [
                        recv_buf[piece, side * 4 + source, half * 2 + part, pl.ds(k, 8, stride=8), :]
                        for source in range(4)
                        for piece in range(blocks)
                    ],
                    axis=0,
                )
                start = pl.multiple_of((half * 8 + k) * RADIX, RADIX)
                spec_ref[part, pl.ds(start, RADIX), pl.ds(side * 128, 128)] = value.T
            return carry

        lax.fori_loop(0, 8, turn, 0)

    def finish():
        gathered(0, own_buf.at[len(slots) - 1])
        x_copy.wait_recv()
        last = len(slots) - 1
        total = own_buf[last, TERMS * plane] + x_recv[TERMS * plane]
        inverse = solve_rows([total[k : k + 1] for k in range(5)], None)

        def tile(step, carry):
            row = step // lane_tiles
            lane = lax.rem(step, lane_tiles)
            rows_at = pl.ds(pl.multiple_of(row * 8, 8), 8)
            lanes_at = pl.ds(pl.multiple_of(lane * 128, 128), 128)
            taylor = [own_buf[last, s * plane + step] + x_recv[s * plane + step] for s in range(TERMS)]
            for t in range(TERMS):
                comp_ref[t, rows_at, lanes_at] = (
                    inverse[t][0] * taylor[0] + inverse[t][1] * taylor[1] + inverse[t][2] * taylor[2]
                )
            return carry

        lax.fori_loop(0, plane, tile, 0)

    for copies in spectrum_copies:
        for copy in copies:
            copy.wait_recv()
    for half in range(halves):
        for part in range(2):
            place(half, part)
    finish()

    for copies in spectrum_copies:
        for copy in copies:
            copy.wait_send()
    for copy in core_copies:
        copy.wait_send()
    for copy in z_copies.values():
        copy.wait_send()
    x_copy.wait_send()


def write_out(comp_ref, spec_ref, comp_hbm, spec_hbm, sem):
    copies = [pltpu.make_async_copy(comp_ref, comp_hbm, sem.at[0])]
    copies += [pltpu.make_async_copy(spec_ref.at[part], spec_hbm.at[part], sem.at[1 + part]) for part in range(2)]
    for copy in copies:
        copy.start()
    for copy in copies:
        copy.wait()


def local(residual, weight_index, weight_table, gridded):
    bands = lax.axis_size("band")
    groups = lax.axis_size("chan")
    count, rows, width = residual.shape
    grid_rows, length = gridded.shape[2:]
    blocks = grid_rows // 8
    tiled = gridded.reshape(2, blocks, 8, RADIX, RADIX)
    tiled = jnp.transpose(tiled, (0, 1, 3, 2, 4)).reshape(2, blocks, RADIX * 8, RADIX)
    columns = width // groups
    out_length = length // bands
    quarters = 2 * (RADIX // bands // 8)
    tiles = TERMS * (rows // 8) * (columns // 128) + 1
    f32 = jnp.float32
    any_space = pl.BlockSpec(memory_space=pl.ANY)
    vmem = pl.BlockSpec(memory_space=pltpu.VMEM)
    dma = pltpu.SemaphoreType.DMA
    slots = 2 * len(SHIFTS)
    components, spectrum = pl.pallas_call(
        body,
        out_shape=(
            pltpu.VMEM((TERMS, rows, columns), f32),
            pltpu.VMEM((2, out_length, grid_rows * bands), f32),
        ),
        in_specs=[any_space] * 6,
        out_specs=(vmem, vmem),
        scratch_shapes=[
            pltpu.SMEM(weight_index.shape, weight_index.dtype),
            pltpu.SMEM(weight_table.shape, f32),
            pltpu.VMEM((4 * RADIX, 2 * RADIX), jnp.bfloat16),
            pltpu.VMEM((2, RADIX, RADIX), f32),
            pltpu.VMEM((2, blocks, RADIX * 8, RADIX), f32),
            pltpu.VMEM((groups, count, rows, columns), f32),
            pltpu.VMEM((bands, blocks, quarters, 64, RADIX), f32),
            pltpu.VMEM((blocks, bands, quarters, 64, RADIX), f32),
            pltpu.VMEM((slots, tiles, 8, 128), f32),
            pltpu.VMEM((slots, tiles, 8, 128), f32),
            pltpu.VMEM((slots, tiles, 8, 128), f32),
            pltpu.VMEM((slots, tiles, 8, 128), f32),
            pltpu.VMEM((tiles, 8, 128), f32),
            pltpu.VMEM((tiles, 8, 128), f32),
            pltpu.SemaphoreType.REGULAR((4,)),
            dma((4,)),
            dma((blocks,)),
            dma((groups,)),
            dma((blocks * bands,)),
            dma((blocks * bands,)),
            dma((slots,)),
            dma((slots,)),
            dma((slots,)),
            dma((slots,)),
            dma,
            dma,
        ],
        compiler_params=pltpu.CompilerParams(
            collective_id=0, has_side_effects=True, vmem_limit_bytes=52 << 20
        ),
    )(residual, weight_index, weight_table, tiled, *(jnp.asarray(table) for table in tables()))
    components, spectrum = pl.pallas_call(
        write_out,
        out_shape=(
            jax.ShapeDtypeStruct(components.shape, f32),
            jax.ShapeDtypeStruct(spectrum.shape, f32),
        ),
        in_specs=[vmem, vmem],
        out_specs=(any_space, any_space),
        scratch_shapes=[dma((3,))],
        compiler_params=pltpu.CompilerParams(vmem_limit_bytes=6 << 20),
    )(*(pltpu.with_memory_space_constraint(array, pltpu.VMEM) for array in (components, spectrum)))
    return (components, spectrum.reshape(2, 1, out_length, grid_rows * bands))


def solution(mesh):
    in_specs = (P("chan", "band", None), P("chan"), P(), P(None, "chan", "band", None))
    out_specs = (P(None, "band", "chan"), P(None, "chan", "band", None))
    return jax.shard_map(local, mesh=mesh, in_specs=in_specs, out_specs=out_specs, check_vma=False)
```

```python
import functools

import jax
import jax.numpy as jnp
import numpy as np
from jax import lax
from jax.experimental import pallas as pl
from jax.experimental.pallas import tpu as pltpu
from jax.sharding import PartitionSpec as P

MESH = pl.DeviceIdType.MESH
RADIX = 128
TERMS = 3
SHIFTS = (2, 1, 3, 0)
READY = 1
FAR = 2


def tables():
    step = np.arange(RADIX)
    angle = 2.0 * np.pi * (np.outer(step, step) % RADIX) / RADIX
    cos, sin = (np.cos(angle), np.sin(angle))
    whole = np.block([[cos, sin], [-sin, cos]]).astype(np.float32)
    high = whole.astype(jnp.bfloat16)
    low = (whole - high.astype(np.float32)).astype(jnp.bfloat16)
    turn = 2.0 * np.pi * np.outer(step, step) / (RADIX * RADIX)
    twist = np.stack([np.cos(turn), -np.sin(turn)]) / RADIX
    return (np.concatenate([high, low]), twist.astype(np.float32))


def three_products(pair, value, axis):
    width = 2 * RADIX
    mul = functools.partial(
        lax.dot_general,
        dimension_numbers=(((1,), (axis,)), ((), ())),
        preferred_element_type=jnp.float32,
    )
    done = []
    for k in range(value.shape[1 - axis] // width):
        cut = slice(k * width, (k + 1) * width)
        tile = value[:, cut] if axis == 0 else value[cut]
        high = tile.astype(jnp.bfloat16)
        low = (tile - high.astype(jnp.float32)).astype(jnp.bfloat16)
        both = mul(pair, high)
        done.append(both[:width] + (both[width:] + mul(pair[:width], low)))
    return jnp.concatenate(done, axis=1)


def solve_rows(moment, taylor):
    m0, m1, m2, m3, m4 = moment
    aa = m2 * m4 - m3 * m3
    ab = m2 * m3 - m1 * m4
    ac = m1 * m3 - m2 * m2
    bb = m0 * m4 - m2 * m2
    bc = m1 * m2 - m0 * m3
    cc = m0 * m2 - m1 * m1
    determ = m0 * aa + m1 * ab + m2 * ac
    aa, ab, ac, bb, bc, cc = (entry / determ for entry in (aa, ab, ac, bb, bc, cc))
    return ((aa, ab, ac), (ab, bb, bc), (ac, bc, cc))


def body(
    res_hbm, index_hbm, table_hbm, grid_hbm, pair_hbm, twist_hbm,
    comp_ref, spec_ref,
    index_ref, table_ref, pair_ref, twist_ref, grid_buf, res_buf, send_buf, recv_buf, core_send, own_buf, core_recv, z_recv, x_send, x_recv,
    word_sem, small_sem, grid_sem, res_sem, a_send, a_recv, c_send, c_recv, z_send_sem, z_recv_sem, x_send_sem, x_recv_sem,
):
    groups = lax.axis_size("chan")
    bands = lax.axis_size("band")
    zs = groups // 4
    chan = lax.axis_index("chan")
    band = lax.axis_index("band")
    x_lo = chan // (2 * zs)
    z_at = (chan // 2) % zs
    core = chan % 2
    ys = bands // 2
    y_at = band // 2
    x_hi = band % 2
    count = res_hbm.shape[0]
    rows = res_hbm.shape[1]
    columns = res_hbm.shape[2] // groups
    row_tiles = rows // 8
    lane_tiles = columns // 128
    plane = row_tiles * lane_tiles
    blocks = grid_hbm.shape[1]
    halves = send_buf.shape[2] // 2

    def chan_of(x, z, c):
        return (x * zs + z) * 2 + c

    def z_of(shift):
        return lax.rem(z_at + shift, zs)

    partner = {"chan": chan_of(x_lo, z_at, 1 - core)}
    across = {"chan": chan_of(1 - x_lo, z_at, core)}

    def along(turn):
        return {"band": lax.rem(y_at + turn, ys) * 2 + x_hi}

    def beyond(turn):
        return {"band": lax.rem(y_at + turn, ys) * 2 + 1 - x_hi}

    def up(turn):
        return {"chan": chan_of(x_lo, z_of(turn), core)}

    nearest = (beyond(0), along(1), along(ys - 1), up(1), up(zs - 1), partner, across)
    barrier = pltpu.get_barrier_semaphore()
    for device in nearest:
        pl.semaphore_signal(barrier, 1, device_id=device, device_id_type=MESH)

    grid_copies = [
        pltpu.make_async_copy(grid_hbm.at[:, k], grid_buf.at[:, k], grid_sem.at[k]) for k in range(blocks)
    ]
    small_copies = [
        pltpu.make_async_copy(source, target, small_sem.at[k])
        for k, (source, target) in enumerate(
            ((pair_hbm, pair_ref), (twist_hbm, twist_ref), (index_hbm, index_ref), (table_hbm, table_ref))
        )
    ]
    for copy in (grid_copies[0], *small_copies, *grid_copies[1:]):
        copy.start()
    slots = [(other, shift) for other in (1, 0) for shift in SHIFTS]
    order = [(away, slot) for away in (1, 0) for slot in range(len(slots))]

    def block_of(away, slot):
        other, shift = slots[slot]
        return chan_of((x_lo + other) % 2, z_of(shift), (core + away) % 2)

    res_copies = []
    for k, (away, slot) in enumerate(order):
        start = pl.multiple_of(block_of(away, slot) * columns, columns)
        res_copies.append(
            pltpu.make_async_copy(res_hbm.at[:, :, pl.ds(start, columns)], res_buf.at[k], res_sem.at[k])
        )

    for copy in small_copies:
        copy.wait()

    def transform(block):
        def taken(part):
            return jnp.concatenate([grid_buf[part, block, pl.ds(k, RADIX, stride=8), :] for k in range(8)], axis=1)

        pair = pair_ref[...]
        stage = three_products(pair, jnp.concatenate([taken(0), taken(1)], axis=0), 0)
        tre, tim = (twist_ref[0], twist_ref[1])
        turned = []
        for k in range(8):
            cut = slice(k * RADIX, (k + 1) * RADIX)
            real, imag = (stage[:RADIX, cut], stage[RADIX:, cut])
            turned.append(jnp.concatenate([real * tre - imag * tim, real * tim + imag * tre], axis=1))
        final = three_products(pair, jnp.concatenate(turned, axis=0), 1)
        for k in range(8):
            for target in range(bands):
                for part in range(2):
                    for half in range(halves):
                        at = part * RADIX + target * (8 * halves) + half * 8
                        send_buf[target, block, half * 2 + part, k * 8 : k * 8 + 8, :] = final[
                            at : at + 8, k * RADIX : (k + 1) * RADIX
                        ]

    def spectrum_copy(piece, length, crossing, turn):
        device = beyond(turn) if crossing else along(turn)
        at = piece * bands + turn * 2 + crossing
        return pltpu.make_async_remote_copy(
            src_ref=send_buf.at[device["band"], pl.ds(piece, length)],
            dst_ref=recv_buf.at[band, pl.ds(piece, length)],
            send_sem=a_send.at[at],
            recv_sem=a_recv.at[at],
            device_id=device,
            device_id_type=MESH,
        )

    ways = [(1, 2), (1, 1), (1, ys - 1), (0, 2), (1, 0), (0, 1), (0, ys - 1)]
    spectrum_copies = [
        [spectrum_copy(piece, 1 if piece <= READY else blocks - 1 - READY, *way) for way in ways]
        for piece in range(READY + 2)
    ]

    def started(pieces, chosen):
        for piece in pieces:
            for way in chosen:
                spectrum_copies[piece][way].start()

    for block in range(blocks):
        grid_copies[block].wait()
        if block == blocks - 1:
            for copy in res_copies:
                copy.start()
        transform(block)
        if block == READY:
            pl.semaphore_wait(barrier, len(nearest))
            pl.semaphore_signal(word_sem.at[0], 1, device_id=beyond(0), device_id_type=MESH)
            pl.semaphore_signal(word_sem.at[1], 1, device_id=along(ys - 1), device_id_type=MESH)
            pl.semaphore_signal(word_sem.at[2], 1, device_id=up(zs - 1), device_id_type=MESH)
            started(range(READY + 1), (4,))
            started((0,), (5, 6))
        if block == FAR:
            pl.semaphore_wait(word_sem.at[1], 1)
            pl.semaphore_signal(word_sem.at[3], 1, device_id=beyond(0), device_id_type=MESH)
            pl.semaphore_wait(word_sem.at[0], 1)
            started((0,), (1, 2, 3))
            started(range(1, READY + 1), (1, 2, 3, 5, 6))
        if block == blocks - 1:
            pl.semaphore_wait(word_sem.at[3], 1)
            pl.semaphore_wait(word_sem.at[2], 1)
            started(range(READY + 1), (0,))
            started((READY + 1,), range(7))

    weights, offsets = ([], [])
    for k in range(count):
        weights.append(table_ref[index_ref[k]])
        position = (chan * count + k).astype(jnp.float32)
        offsets.append((2.0 * position + 1.0) / (count * groups) - 1.0)
    coeffs = [weights, [w * o for w, o in zip(weights, offsets)], [w * o * o for w, o in zip(weights, offsets)]]
    powers = list(weights)
    moments = []
    for power in range(5):
        total = powers[0]
        for k in range(1, count):
            total = total + powers[k]
        moments.append(total)
        powers = [p * o for p, o in zip(powers, offsets)]
    sublane = lax.broadcasted_iota(jnp.int32, (8, 128), 0)
    moment_tile = jnp.zeros((8, 128), jnp.float32)
    for power in range(5):
        moment_tile = jnp.where(sublane == power, moments[power], moment_tile)

    def sums(k, target_ref, slot, extra):
        res_copies[k].wait()

        def tile(step, carry):
            row = step // lane_tiles
            lane = lax.rem(step, lane_tiles)
            rows_at = pl.ds(pl.multiple_of(row * 8, 8), 8)
            lanes_at = pl.ds(pl.multiple_of(lane * 128, 128), 128)
            totals = [None] * TERMS
            for channel in range(count):
                value = res_buf[k, channel, rows_at, lanes_at]
                for term in range(TERMS):
                    product = value * coeffs[term][channel]
                    totals[term] = product if totals[term] is None else totals[term] + product
            for term in range(TERMS):
                at = term * plane + step
                total = totals[term]
                if extra is not None:
                    total = total + extra[slot, at]
                target_ref[slot, at] = total
            return carry

        lax.fori_loop(0, plane, tile, 0, unroll=4)
        moment = moment_tile
        if extra is not None:
            moment = moment + extra[slot, TERMS * plane]
        target_ref[slot, TERMS * plane] = moment

    core_copies = []
    for slot in range(len(slots)):
        sums(slot, core_send, slot, None)
        copy = pltpu.make_async_remote_copy(
            src_ref=core_send.at[slot],
            dst_ref=core_recv.at[slot],
            send_sem=c_send.at[slot],
            recv_sem=c_recv.at[slot],
            device_id=partner,
            device_id_type=MESH,
        )
        copy.start()
        core_copies.append(copy)

    z_copies = {}
    for slot, (other, shift) in enumerate(slots):
        core_copies[slot].wait_recv()
        sums(len(slots) + slot, own_buf, slot, core_recv)
        if shift:
            copy = pltpu.make_async_remote_copy(
                src_ref=own_buf.at[slot],
                dst_ref=z_recv.at[slot],
                send_sem=z_send_sem.at[slot],
                recv_sem=z_recv_sem.at[slot],
                device_id={"chan": chan_of(x_lo, z_of(shift), core)},
                device_id_type=MESH,
            )
            copy.start()
            z_copies[slot] = copy

    own = send_buf.at[band]
    for piece in range(blocks):
        recv_buf[band, piece] = own[piece]

    def gathered(other, target):
        base = [k for k, key in enumerate(slots) if key == (other, 0)][0]
        came = [k for k, key in enumerate(slots) if key[0] == other and key[1]]
        for slot in came:
            z_copies[slot].wait_recv()

        def tile(step, carry):
            total = own_buf[base, step]
            for slot in came:
                total = total + z_recv[slot, step]
            target[step] = total
            return carry

        lax.fori_loop(0, TERMS * plane + 1, tile, 0)

    gathered(1, x_send)
    x_copy = pltpu.make_async_remote_copy(
        src_ref=x_send,
        dst_ref=x_recv,
        send_sem=x_send_sem,
        recv_sem=x_recv_sem,
        device_id=across,
        device_id_type=MESH,
    )
    x_copy.start()

    def place(half, part):
        def turn(k, carry):
            for side in range(2):
                value = jnp.concatenate(
                    [
                        recv_buf[side * 4 + source, piece, half * 2 + part, pl.ds(k, 8, stride=8), :]
                        for source in range(4)
                        for piece in range(blocks)
                    ],
                    axis=0,
                )
                start = pl.multiple_of((half * 8 + k) * RADIX, RADIX)
                spec_ref[part, pl.ds(start, RADIX), pl.ds(side * 128, 128)] = value.T
            return carry

        lax.fori_loop(0, 8, turn, 0)

    def finish():
        gathered(0, own_buf.at[len(slots) - 1])
        x_copy.wait_recv()
        last = len(slots) - 1
        total = own_buf[last, TERMS * plane] + x_recv[TERMS * plane]
        inverse = solve_rows([total[k : k + 1] for k in range(5)], None)

        def tile(step, carry):
            row = step // lane_tiles
            lane = lax.rem(step, lane_tiles)
            rows_at = pl.ds(pl.multiple_of(row * 8, 8), 8)
            lanes_at = pl.ds(pl.multiple_of(lane * 128, 128), 128)
            taylor = [own_buf[last, s * plane + step] + x_recv[s * plane + step] for s in range(TERMS)]
            for t in range(TERMS):
                comp_ref[t, rows_at, lanes_at] = (
                    inverse[t][0] * taylor[0] + inverse[t][1] * taylor[1] + inverse[t][2] * taylor[2]
                )
            return carry

        lax.fori_loop(0, plane, tile, 0)

    for copies in spectrum_copies:
        for copy in copies:
            copy.wait_recv()
    for half in range(halves):
        for part in range(2):
            place(half, part)
    finish()

    for copies in spectrum_copies:
        for copy in copies:
            copy.wait_send()
    for copy in core_copies:
        copy.wait_send()
    for copy in z_copies.values():
        copy.wait_send()
    x_copy.wait_send()


def write_out(comp_ref, spec_ref, comp_hbm, spec_hbm, sem):
    copies = [pltpu.make_async_copy(comp_ref, comp_hbm, sem.at[0])]
    copies += [pltpu.make_async_copy(spec_ref.at[part], spec_hbm.at[part], sem.at[1 + part]) for part in range(2)]
    for copy in copies:
        copy.start()
    for copy in copies:
        copy.wait()


def local(residual, weight_index, weight_table, gridded):
    bands = lax.axis_size("band")
    groups = lax.axis_size("chan")
    count, rows, width = residual.shape
    grid_rows, length = gridded.shape[2:]
    blocks = grid_rows // 8
    tiled = gridded.reshape(2, blocks, 8, RADIX, RADIX)
    tiled = jnp.transpose(tiled, (0, 1, 3, 2, 4)).reshape(2, blocks, RADIX * 8, RADIX)
    columns = width // groups
    out_length = length // bands
    quarters = 2 * (RADIX // bands // 8)
    tiles = TERMS * (rows // 8) * (columns // 128) + 1
    f32 = jnp.float32
    any_space = pl.BlockSpec(memory_space=pl.ANY)
    vmem = pl.BlockSpec(memory_space=pltpu.VMEM)
    dma = pltpu.SemaphoreType.DMA
    slots = 2 * len(SHIFTS)
    components, spectrum = pl.pallas_call(
        body,
        out_shape=(
            pltpu.VMEM((TERMS, rows, columns), f32),
            pltpu.VMEM((2, out_length, grid_rows * bands), f32),
        ),
        in_specs=[any_space] * 6,
        out_specs=(vmem, vmem),
        scratch_shapes=[
            pltpu.SMEM(weight_index.shape, weight_index.dtype),
            pltpu.SMEM(weight_table.shape, f32),
            pltpu.VMEM((4 * RADIX, 2 * RADIX), jnp.bfloat16),
            pltpu.VMEM((2, RADIX, RADIX), f32),
            pltpu.VMEM((2, blocks, RADIX * 8, RADIX), f32),
            pltpu.VMEM((groups, count, rows, columns), f32),
            pltpu.VMEM((bands, blocks, quarters, 64, RADIX), f32),
            pltpu.VMEM((bands, blocks, quarters, 64, RADIX), f32),
            pltpu.VMEM((slots, tiles, 8, 128), f32),
            pltpu.VMEM((slots, tiles, 8, 128), f32),
            pltpu.VMEM((slots, tiles, 8, 128), f32),
            pltpu.VMEM((slots, tiles, 8, 128), f32),
            pltpu.VMEM((tiles, 8, 128), f32),
            pltpu.VMEM((tiles, 8, 128), f32),
            pltpu.SemaphoreType.REGULAR((4,)),
            dma((4,)),
            dma((blocks,)),
            dma((groups,)),
            dma((blocks * bands,)),
            dma((blocks * bands,)),
            dma((slots,)),
            dma((slots,)),
            dma((slots,)),
            dma((slots,)),
            dma,
            dma,
        ],
        compiler_params=pltpu.CompilerParams(
            collective_id=0, has_side_effects=True, vmem_limit_bytes=52 << 20
        ),
    )(residual, weight_index, weight_table, tiled, *(jnp.asarray(table) for table in tables()))
    components, spectrum = pl.pallas_call(
        write_out,
        out_shape=(
            jax.ShapeDtypeStruct(components.shape, f32),
            jax.ShapeDtypeStruct(spectrum.shape, f32),
        ),
        in_specs=[vmem, vmem],
        out_specs=(any_space, any_space),
        scratch_shapes=[dma((3,))],
        compiler_params=pltpu.CompilerParams(vmem_limit_bytes=6 << 20),
    )(*(pltpu.with_memory_space_constraint(array, pltpu.VMEM) for array in (components, spectrum)))
    return (components, spectrum.reshape(2, 1, out_length, grid_rows * bands))


def solution(mesh):
    in_specs = (P("chan", "band", None), P("chan"), P(), P(None, "chan", "band", None))
    out_specs = (P(None, "band", "chan"), P(None, "chan", "band", None))
    return jax.shard_map(local, mesh=mesh, in_specs=in_specs, out_specs=out_specs, check_vma=False)
```
